512 devices in a mesh: inline: 32 (over z, y_hi), xline: 16 (over y_lo, x, core).
Axes of the slice: x: 4, y: 4 (y_hi: 2, y_lo: 2; y = y_hi * 2 + y_lo), z: 16, core: 2. Of those that a mesh axis runs over, the one named last changes fastest.
Arguments:
- samples: float32 [2, 32, 16384], P(None, 'inline', 'xline'), may hold values from -6 to 6
Outputs:
- values: float32 [2, 131072], P(None, ('inline', 'xline'))
The draws below stay inside these ranges and needn't reach their ends.
All inputs are finite; a program needn't handle non-finite values.
Results may differ from the reference program's by a relative error of at most 0.0003.
Values sent between devices are 32-bit elements; how exact they have to be, the bound alone decides.
No kernel may reach another device: no remote copies, remote signals or barrier semaphores. Data moves between devices by JAX's collectives and lax.ppermute only.
A program may use at most 64 MiB of HBM per device.

```python
import math
import jax
import jax.numpy as jnp
from jax import lax

GI = 1
GC = 4
NF = 256
COLS = 256
NI = 32
NCF = 16384
N_INLINE = 32
N_XLINE = 16


def level_of(rng, dims, cuts, low, largest):
    loudness, own = 1.0, jax.random.fold_in(rng, 6)
    for dim, blocks in cuts:
        draws = jnp.exp(jax.random.uniform(jax.random.fold_in(own, dim), (blocks,), jnp.float32, low / len(cuts), largest / len(cuts)))
        loudness = loudness * jnp.repeat(draws, dims[dim] // blocks).reshape([-1 if axis == dim else 1 for axis in range(len(dims))])
    return loudness


def scatter_about(own_key, dims, scale, most, shards=(), held_as=jnp.bfloat16):
    values = jax.random.normal(own_key, dims, jnp.float32) * scale
    if len(shards) > 0:
        values = level_of(own_key, dims, shards, -0.22, 0.18) * values
    return jnp.clip(values, min=-most, max=most).astype(held_as)


def setup_inputs(seed: int = 0) -> dict:
    keys = jax.random.split(jax.random.key(seed), 2)
    samples = scatter_about(keys[0], (2, NI, NCF), 1.0, 6.0, ((1, 32), (2, 16)), jnp.float32)
    return {"samples": samples}


KAPPA = 40.0
HIGH = lax.Precision.HIGHEST

def cheb_nodes():
    node_order = jnp.arange(5, dtype=jnp.float32)
    return 0.5 * jnp.cos(node_order * (math.pi / 4.0))

def lagrange(points):
    node_list = cheb_nodes()
    basis_rows = []
    for node_index in range(5):
        factor = jnp.ones_like(points)
        for other_node in range(5):
            if other_node != node_index:
                factor = factor * (points - node_list[other_node]) / (node_list[node_index] - node_list[other_node])
        basis_rows.append(factor)
    return jnp.stack(basis_rows)

def box_points(inline_low, inline_width, xline_low, xline_width):
    shifted = cheb_nodes() + 0.5
    grid_shape = (5, 5, 5)
    along_inline = jnp.broadcast_to((inline_low + inline_width * shifted)[:, None, None], grid_shape).reshape(125)
    along_xline = jnp.broadcast_to((xline_low + xline_width * shifted)[None, :, None], grid_shape).reshape(125)
    frequency = jnp.broadcast_to(shifted[None, None, :], grid_shape).reshape(125)
    return (along_inline, along_xline, frequency)

def traveltime(points, centers):
    offset_inline, offset_xline, frequency = points
    anchor = 0.5 + centers[0][None, :]
    radicand = anchor * anchor + centers[1][None, :] * (offset_inline * offset_inline)[:, None]
    radicand = radicand + centers[2][None, :] * (offset_xline * offset_xline)[:, None]
    return KAPPA * (0.5 + frequency)[:, None] * jnp.sqrt(radicand)

def finish(summed, parent_span, centers):
    phase_angle = traveltime(box_points(parent_span[0], parent_span[1], parent_span[2], parent_span[3]), centers)
    cosine = jnp.cos(phase_angle)
    sine_vals = jnp.sin(phase_angle)
    return jnp.stack([summed[0] * cosine + summed[1] * sine_vals, summed[1] * cosine - summed[0] * sine_vals])

def child_term(weights, child_side, axis_pick, parent_span, children):
    inline_low, inline_width, xline_low, xline_width = parent_span
    if axis_pick == 0:
        phase_angle = traveltime(box_points(inline_low + 0.5 * inline_width * child_side, 0.5 * inline_width, xline_low, xline_width), children)
    else:
        phase_angle = traveltime(box_points(inline_low, inline_width, xline_low + 0.5 * xline_width * child_side, 0.5 * xline_width), children)
    cosine = jnp.cos(phase_angle)
    sine_vals = jnp.sin(phase_angle)
    real_in = jnp.concatenate([weights[0], weights[0]], axis=1)
    imag_in = jnp.concatenate([weights[1], weights[1]], axis=1)
    stacked = jnp.stack([cosine * real_in - sine_vals * imag_in, sine_vals * real_in + cosine * imag_in])
    stacked = stacked.reshape(2, 5, 5, 5, -1)
    matrix = lagrange((child_side - 0.5) * 0.5 + 0.5 * cheb_nodes())
    if axis_pick == 0:
        mixed = jnp.einsum('ab,rbcdn->racdn', matrix, stacked, precision=HIGH)
    else:
        mixed = jnp.einsum('ab,rcbdn->rcadn', matrix, stacked, precision=HIGH)
    return mixed.reshape(2, 125, -1)

def parent_box(inline_pos, xline_pos, inline_count, xline_count, merged, axis_pick):
    inline_bits = merged[0] + (1 if axis_pick == 0 else 0)
    xline_bits = merged[1] + (1 if axis_pick == 1 else 0)
    inline_low = (inline_pos >> inline_bits << inline_bits).astype(jnp.float32) / inline_count
    xline_low = (xline_pos >> xline_bits << xline_bits).astype(jnp.float32) / xline_count
    return (inline_low, 2.0 ** inline_bits / inline_count, xline_low, 2.0 ** xline_bits / xline_count)

def roster(inline_count, xline_count):
    inline_bits = inline_count.bit_length() - 1
    xline_bits = xline_count.bit_length() - 1
    level_plan = []
    for level_num in range(max(inline_bits, xline_bits)):
        if level_num < inline_bits:
            level_plan.append((0, level_num))
        if level_num < xline_bits:
            level_plan.append((1, level_num))
    return level_plan

def split_counts(column_count):
    tree_depth = (column_count - 1).bit_length()
    return (tree_depth, [len([depth_step for depth_step in range(tree_depth) if depth_step % 3 == axis_num]) for axis_num in range(3)])

def initial_centers(column_count):
    tree_depth = (column_count - 1).bit_length()
    column = jnp.arange(column_count, dtype=jnp.int32)
    coords = []
    for axis_num in range(3):
        splits = [depth_step for depth_step in range(tree_depth) if depth_step % 3 == axis_num]
        coord = jnp.full((column_count,), 0.5 * 0.5 ** len(splits), jnp.float32)
        for split_rank, depth_step in enumerate(splits):
            digit = column >> tree_depth - 1 - depth_step & 1
            coord = coord + digit.astype(jnp.float32) * 0.5 ** (split_rank + 1)
        coords.append(coord)
    return jnp.stack(coords)

def split_targets(centers, split_dim, span_width):
    offsets = [0.0, 0.0, 0.0]
    offsets[split_dim] = 0.25 * span_width
    shift_col = jnp.array(offsets, dtype=jnp.float32)[:, None]
    return jnp.concatenate([centers - shift_col, centers + shift_col], axis=1)

def leaf_weights(flat_samples, inline_pos, xline_pos, inline_count, xline_count, centers, count_inline, count_xline, freq_count):
    z_inline = (jnp.arange(count_inline, dtype=jnp.float32) + 0.5) / count_inline - 0.5
    z_xline = (jnp.arange(count_xline, dtype=jnp.float32) + 0.5) / count_xline - 0.5
    z_freq = (jnp.arange(freq_count, dtype=jnp.float32) + 0.5) / freq_count - 0.5
    basis_rest = jnp.einsum('bc,df->bdcf', lagrange(z_xline), lagrange(z_freq), precision=HIGH).reshape(25, -1)
    inline_basis = lagrange(z_inline).T
    inline_low = inline_pos.astype(jnp.float32) / inline_count
    xline_low = xline_pos.astype(jnp.float32) / xline_count
    grid_shape = (count_xline, freq_count)
    sample_xline = jnp.broadcast_to((xline_low + (z_xline + 0.5) / xline_count)[:, None], grid_shape).reshape(-1)
    sample_freq = jnp.broadcast_to((z_freq + 0.5)[None, :], grid_shape).reshape(-1)
    row_samples = flat_samples.reshape(2, count_inline, -1).transpose(1, 0, 2)
    row_inline = inline_low + (z_inline + 0.5) / inline_count
    column_count = centers.shape[1]

    def add_row(total, items):
        row_pair, inline_coord, row_basis = items
        coord_vec = jnp.zeros_like(sample_freq) + inline_coord
        phase_angle = traveltime((coord_vec, sample_xline, sample_freq), centers)
        cosine = jnp.cos(phase_angle)
        sine_vals = jnp.sin(phase_angle)
        real_in = row_pair[0][:, None]
        imag_in = row_pair[1][:, None]
        real_part = jnp.dot(basis_rest, cosine * real_in - sine_vals * imag_in, precision=HIGH)
        imag_part = jnp.dot(basis_rest, sine_vals * real_in + cosine * imag_in, precision=HIGH)
        pair = jnp.stack([real_part, imag_part])
        spread = row_basis[None, :, None, None] * pair[:, None, :, :]
        return (total + spread.reshape(2, 125, column_count), None)
    start_total = jnp.zeros((2, 125, column_count), dtype=jnp.float32)
    summed, unused = lax.scan(add_row, start_total, (row_samples, row_inline, inline_basis))
    leaf_span = (inline_low, 1.0 / inline_count, xline_low, 1.0 / xline_count)
    return finish(summed, leaf_span, centers)

def reference(samples):
    inline_count = N_INLINE
    xline_count = N_XLINE
    devices = inline_count * xline_count
    flat_samples = samples.reshape(2, inline_count, GI, xline_count, GC * NF)
    flat_samples = flat_samples.transpose(1, 3, 0, 2, 4).reshape(devices, 2, GI * GC * NF)
    device_ids = jnp.arange(devices, dtype=jnp.int32)
    inline_index = device_ids // xline_count
    xline_index = device_ids % xline_count
    start_centers = initial_centers(COLS)

    def leaf_one(items):
        return leaf_weights(items[0], items[1], items[2], inline_count, xline_count, start_centers, GI, GC, NF)
    weights = lax.map(leaf_one, (flat_samples, inline_index, xline_index))
    centers = jnp.broadcast_to(start_centers[None], (devices, 3, COLS))
    tree_depth, counts = split_counts(COLS)
    half_cols = COLS // 2
    merged = [0, 0]
    level_plan = roster(inline_count, xline_count)
    for position, (axis_pick, bit_place) in enumerate(level_plan):
        split_dim = tree_depth % 3
        span_width = 0.5 ** counts[split_dim]
        is_last = position == len(level_plan) - 1
        shift_bits = bit_place + (xline_count.bit_length() - 1 if axis_pick == 0 else 0)
        partner = device_ids ^ 1 << shift_bits
        axis_index = inline_index if axis_pick == 0 else xline_index
        own_bits = axis_index >> bit_place & 1
        partner_weights = jnp.take(weights, partner, axis=0)
        merged_now = list(merged)

        def level_one(own_weights, far_weights, own_centers, own_bit, inline_pos, xline_pos):
            keep_start = (own_bit * half_cols).astype(jnp.int32)
            parent_span = parent_box(inline_pos, xline_pos, inline_count, xline_count, merged_now, axis_pick)
            children = split_targets(lax.dynamic_slice_in_dim(own_centers, keep_start, half_cols, 1), split_dim, span_width)
            own_child = own_bit.astype(jnp.float32)
            own_term = child_term(lax.dynamic_slice_in_dim(own_weights, keep_start, half_cols, 2), own_child, axis_pick, parent_span, children)
            far_term = child_term(lax.dynamic_slice_in_dim(far_weights, keep_start, half_cols, 2), 1.0 - own_child, axis_pick, parent_span, children)
            summed = own_term + far_term
            if is_last:
                return (lax.optimization_barrier(jnp.sum(summed, axis=1)), children)
            return (finish(summed, parent_span, children), children)
        weights, centers = jax.vmap(level_one)(weights, partner_weights, centers, own_bits, inline_index, xline_index)
        merged[axis_pick] += 1
        counts[split_dim] += 1
        tree_depth += 1
    sample_norm = 1.0 / math.sqrt(GI * GC * NF * devices)
    return weights.transpose(1, 0, 2).reshape(2, devices * COLS) * sample_norm
```

```python
import math

import jax
import jax.numpy as jnp
import numpy as np
from jax import lax
from jax.experimental import pallas as pl
from jax.experimental.pallas import tpu as pltpu
from jax.sharding import PartitionSpec as P

NF = 256
COLS = 256
GC = 4
N_INLINE = 32
N_XLINE = 16
KAPPA = 40.0
AXES = ("inline", "xline")
F32 = jnp.float32
BF16 = jnp.bfloat16

NODES = 0.5 * np.cos(np.arange(5) * (math.pi / 4.0))


def basis_at(points):
    rows = []
    for k in range(5):
        factor = np.ones_like(points)
        for j in range(5):
            if j != k:
                factor = factor * (points - NODES[j]) / (NODES[k] - NODES[j])
        rows.append(factor)
    return np.stack(rows)


CHILD = [basis_at((t - 0.5) * 0.5 + 0.5 * NODES) for t in (0, 1)]
LEAF_INLINE = basis_at(np.array([0.0]))[:, 0]
LEAF_XLINE = basis_at((np.arange(GC) + 0.5) / GC - 0.5)


def gather_groups():
    groups = []
    for base in range(N_INLINE * N_XLINE):
        a, b = base // N_XLINE, base % N_XLINE
        if a & 3 or b & 3:
            continue
        members = []
        for j in range(16):
            a0, b0, a1, b1 = j >> 3 & 1, j >> 2 & 1, j >> 1 & 1, j & 1
            members.append((a | a0 | a1 << 1) * N_XLINE + (b | b0 | b1 << 1))
        groups.append(members)
    return groups


def scatter_groups():
    groups = []
    for base in range(N_INLINE * N_XLINE):
        a, b = base // N_XLINE, base % N_XLINE
        if a >> 2 or b >> 2:
            continue
        members = []
        for j in range(32):
            k6, k7, k5, k3, k4 = j >> 4 & 1, j >> 3 & 1, j >> 2 & 1, j >> 1 & 1, j & 1
            members.append(
                (a | k3 << 2 | k5 << 3 | k7 << 4) * N_XLINE + (b | k4 << 2 | k6 << 3)
            )
        groups.append(members)
    return groups


def series(scale, bound, odd):
    coefs = []
    n = 0
    while True:
        power = 2 * n + (1 if odd else 0)
        size = (scale * bound) ** power / math.factorial(power)
        if size < 1e-8:
            return coefs
        coefs.append((-1.0) ** n * scale**power / math.factorial(power))
        n += 1


def poly(coefs, square):
    total = square * coefs[-1] + coefs[-2]
    for coef in coefs[-3::-1]:
        total = total * square + coef
    return total


def sincos_small(r, scale, bound):
    square = r * r
    return r * poly(series(scale, bound, True), square), poly(series(scale, bound, False), square)


def sincos_wide(x):
    turns = jnp.floor(x * (2.0 / math.pi) + 0.5)
    r = x - turns * 1.5703125
    r = r - turns * 4.837512969970703125e-4
    r = r - turns * 7.54978995489188216e-8
    sine, cosine = sincos_small(r, 1.0, 0.8)
    quarter = turns.astype(jnp.int32)
    swap = (quarter & 1) == 1
    s = jnp.where(swap, cosine, sine)
    c = jnp.where(swap, sine, cosine)
    s = jnp.where((quarter & 2) == 2, -s, s)
    c = jnp.where(((quarter + 1) & 2) == 2, -c, c)
    return s, c


def cmul(ar, ai, br, bi):
    return ar * br - ai * bi, ar * bi + ai * br


def full(value):
    return jnp.full((8, 128), value, F32)


def kernel(where_ref, rows_ref, out_ref, v_ref, tab_ref, leaf_ref, p_ref, q_ref, wa_ref, wb_ref, x_ref):
    a = where_ref[0]
    b = where_ref[1]
    lane = lax.broadcasted_iota(jnp.int32, (8, 128), 1)
    sub = lax.broadcasted_iota(jnp.int32, (8, 128), 0)
    bit2 = sub >> 2 & 1
    bit1 = sub >> 1 & 1
    bit0 = sub & 1

    left = lax.broadcasted_iota(jnp.int32, (16, 8, 128), 2) < 64
    re = rows_ref[:, 0:8, :]
    im = rows_ref[:, 8:16, :]
    re_r = pltpu.roll(re, 64, 2)
    im_r = pltpu.roll(im, 64, 2)
    v_ref[0, 0] = jnp.where(left, re, -im_r)
    v_ref[1, 0] = jnp.where(left, re_r, -im)
    v_ref[0, 1] = jnp.where(left, im, re_r)
    v_ref[1, 1] = jnp.where(left, im_r, re)

    column = lane + ((a & 1) << 7)

    def digits(places):
        coord = full(0.5 * 0.5 ** len(places))
        for rank, place in enumerate(places):
            coord = coord + (column >> place & 1).astype(F32) * 0.5 ** (rank + 1)
        return coord

    g0 = digits((7, 4, 1))
    g1 = digits((6, 3, 0))
    g2 = digits((5, 2))

    def sign_of(bit):
        return (2 * bit - 1).astype(F32)

    a_base = a & ~3
    b_base = b & ~3

    for half in range(2):
        box_a = (a_base + half + 2 * bit1).astype(F32)
        box_b = (b_base + bit2 + 2 * bit0).astype(F32)
        x0 = (box_a + 0.5) * (1.0 / N_INLINE)
        part = (0.5 + g0) * (0.5 + g0) + g1 * (x0 * x0)
        for c in range(GC):
            at = pl.ds(c * 16 + half * 8, 8)
            x1 = (box_b + (c + 0.5) / GC) * (1.0 / N_XLINE)
            radicand = part + g2 * (x1 * x1)
            step = (KAPPA / NF) * jnp.sqrt(radicand)
            tab_ref[0, at, :] = step
            s, co = sincos_wide(step * 132.0)
            s64, c64 = sincos_wide(step * 64.0)
            for f1 in range(4):
                tab_ref[1 + 2 * f1, at, :] = co
                tab_ref[2 + 2 * f1, at, :] = s
                if f1 < 3:
                    co, s = cmul(co, s, c64, s64)
            s8, c8 = sincos_wide(step * 8.0)
            co, s = c8, s8
            for f2 in range(1, 8):
                tab_ref[7 + 2 * f2, at, :] = co
                tab_ref[8 + 2 * f2, at, :] = s
                if f2 < 7:
                    co, s = cmul(co, s, c8, s8)

    basis = []
    for f1 in range(4):
        z = ((lane & 63).astype(F32) + (f1 * 64 + 0.5)) * (1.0 / NF) - 0.5
        factor = jnp.zeros((8, 128), F32)
        for k in range(5):
            scale = 1.0
            for j in range(5):
                if j != k:
                    scale = scale / (NODES[k] - NODES[j])
            factor = jnp.where(sub == k, scale, factor)
        for j in range(5):
            factor = factor * jnp.where(sub == j, 1.0, z - NODES[j])
        basis.append(factor)

    offset = sub.astype(F32) - 3.5

    def leaf_box(box, carry):
        totals = []
        for c in range(GC):
            row = c * 16 + box

            def table(i):
                return jnp.broadcast_to(tab_ref[i, pl.ds(row, 1), :], (8, 128))

            s_a, c_a = sincos_small(table(0) * offset, 1.0, 1.15)
            cos_rows, sin_rows = [c_a], [s_a]
            for f2 in range(1, 8):
                cr, sr = cmul(c_a, s_a, table(7 + 2 * f2), table(8 + 2 * f2))
                cos_rows.append(cr)
                sin_rows.append(sr)
            right = jnp.concatenate(cos_rows + sin_rows, axis=0)
            right_hi = right.astype(BF16)
            right_lo = (right - right_hi.astype(F32)).astype(BF16)
            rows = []
            for f1 in range(4):
                for part in range(2):
                    sample = v_ref[f1 & 1, part, pl.ds(box, 1), 2 * c + f1 // 2, :]
                    rows.append(basis[f1] * jnp.broadcast_to(sample, (8, 128)))
            lhs = jnp.concatenate(rows, axis=0)
            lhs_hi = lhs.astype(BF16)
            lhs_lo = (lhs - lhs_hi.astype(F32)).astype(BF16)
            both = jnp.concatenate([lhs_hi, lhs_hi], axis=1)
            mixed = jnp.dot(both, jnp.concatenate([right_hi, right_lo], axis=0), preferred_element_type=F32)
            mixed = mixed + jnp.dot(lhs_lo, right_hi, preferred_element_type=F32)
            t_re = None
            for f1 in range(4):
                u_re = mixed[f1 * 16 : f1 * 16 + 8]
                u_im = mixed[f1 * 16 + 8 : f1 * 16 + 16]
                r_re, r_im = cmul(u_re, u_im, table(1 + 2 * f1), table(2 + 2 * f1))
                t_re, t_im = (r_re, r_im) if t_re is None else (t_re + r_re, t_im + r_im)
            totals.append((t_re, t_im))
        for a1 in range(5):
            for part in range(2):
                total = totals[0][part] * float(LEAF_XLINE[a1, 0])
                for c in range(1, GC):
                    total = total + totals[c][part] * float(LEAF_XLINE[a1, c])
                leaf_ref[pl.ds((a1 * 16 + part) * 16 + box, 8, stride=32), :] = total
        return carry

    lax.fori_loop(0, 16, leaf_box, 0)

    def squares(low, width):
        return [(low + width * (float(NODES[k]) + 0.5)) * (low + width * (float(NODES[k]) + 0.5)) for k in range(5)]

    def prepare(low0, width0, low1, width1, slot=0):
        x0 = squares(low0, width0)
        x1 = squares(low1, width1)
        for k in range(5):
            p_ref[slot, k] = full(0.0) + x0[k]
            q_ref[slot, k] = full(0.0) + x1[k]

    def factors(anchor_sq, centre, slot, b0, b1, dim, move, bound):
        xx0 = p_ref[slot, b0]
        xx1 = q_ref[slot, b1]
        radicand = anchor_sq + centre[1] * xx0 + centre[2] * xx1
        root = radicand * lax.rsqrt(radicand)
        result = []
        for sigma in move:
            if dim == 0:
                moved = radicand + sigma
            elif dim == 1:
                moved = radicand + sigma * xx0
            else:
                moved = radicand + sigma * xx1
            change = moved * lax.rsqrt(moved) - root
            s_u, c_u = sincos_small(change, 0.5 * KAPPA, bound)
            s_v, c_v = sincos_small(change, KAPPA * float(NODES[1]), bound)
            result.append((c_u, s_u, c_v, s_v))
        return result

    def five(factor):
        c1, s1, cv, sv = factor
        c2 = c1 * c1 - s1 * s1
        s2 = c1 * s1
        s2 = s2 + s2
        c3, s3 = cmul(c2, s2, c1, s1)
        cc, ss, cs, sc = c2 * cv, s2 * sv, c2 * sv, s2 * cv
        return [(c3, s3), (cc - ss, sc + cs), (c2, s2), (cc + ss, sc - cs), (c1, s1)]

    def moves(centre, dim, q, sigmas):
        if dim == 0:
            return [2.0 * q * sigma * (0.5 + centre[0]) + q * q for sigma in sigmas]
        return [q * sigma + full(0.0) for sigma in sigmas]

    def merge(axis, dim, q, sides, centre, sigmas, read, write, combine):
        anchor = 0.5 + centre[0]
        anchor_sq = anchor * anchor
        step = moves(centre, dim, q, sigmas)

        def body(other, carry):
            for m in range(len(sigmas)):
                pass
            for side, (slot, coef) in enumerate(sides):
                for b in range(5):
                    b0, b1 = (b, other) if axis == 0 else (other, b)
                    made = factors(anchor_sq, centre, slot, b0, b1, dim, step, q)
                    turns = [five(item) for item in made]
                    for b2 in range(5):
                        w_re, w_im = read(side, b0, b1, b2)
                        for m in range(len(sigmas)):
                            x_re, x_im = cmul(w_re, w_im, turns[m][b2][0], turns[m][b2][1])
                            at = ((m * 2 + side) * 5 + b) * 10 + b2 * 2
                            x_ref[at] = x_re
                            x_ref[at + 1] = x_im
            for m in range(len(sigmas)):
                for comp in range(10):
                    for i in range(5):
                        total = None
                        for side, (slot, coef) in enumerate(sides):
                            for b in range(5):
                                item = x_ref[((m * 2 + side) * 5 + b) * 10 + comp] * coef(i, b)
                                total = item if total is None else total + item
                        i0, i1 = (i, other) if axis == 0 else (other, i)
                        write(m, i0, i1, comp, combine(total))
            return carry

        lax.fori_loop(0, 5, body, 0)

    def chosen(mask):
        table = [
            [jnp.where(mask, float(CHILD[1][i, j]), float(CHILD[0][i, j])) for j in range(5)]
            for i in range(5)
        ]
        return lambda i, j: table[i][j]

    def state_reader(ref, index):
        def read(side, b0, b1, b2):
            at = (b0 * 5 + b1) * 10 + b2 * 2
            return ref[index, at], ref[index, at + 1]

        return read

    def state_writer(ref, index_of):
        def write(m, i0, i1, comp, value):
            ref[index_of(m), (i0 * 5 + i1) * 10 + comp] = value

        return write

    unit_b = (b_base + bit2 + 2 * bit0).astype(F32) * (1.0 / N_XLINE)
    unit_a = (a_base + 2 * bit1).astype(F32) * (1.0 / N_INLINE)
    prepare(unit_a, 1.0 / N_INLINE, unit_b, 1.0 / N_XLINE, 0)
    prepare(unit_a + 1.0 / N_INLINE, 1.0 / N_INLINE, unit_b, 1.0 / N_XLINE, 1)

    def leaf_read(side, b0, b1, b2):
        base = (b1 * 8 + b2) * 32 + side * 8
        if not isinstance(base, int):
            base = pl.multiple_of(base, 8)
        return leaf_ref[pl.ds(base, 8), :], leaf_ref[pl.ds(base + 16, 8), :]

    merge(
        0, 2, 2.0**-4,
        [
            (t, (lambda t: lambda i, j: float(CHILD[t][i, j] * LEAF_INLINE[j]))(t))
            for t in (0, 1)
        ],
        (g0, g1, g2), [sign_of(full(0).astype(jnp.int32) + (b & 1))],
        leaf_read, state_writer(wa_ref, lambda m: 0), lambda v: v,
    )
    g2 = g2 + sign_of(b & 1) * 2.0**-4

    prepare(unit_a, 2.0 / N_INLINE, unit_b, 1.0 / N_XLINE)
    merge(
        1, 0, 2.0**-5, [(0, chosen(bit2 == 1))], (g0, g1, g2),
        [sign_of(full(0).astype(jnp.int32) + (a >> 1 & 1))],
        state_reader(wa_ref, 0), state_writer(wb_ref, lambda m: 0),
        lambda v: v + pltpu.roll(v, 4, 0),
    )
    g0 = g0 + sign_of(a >> 1 & 1) * 2.0**-5

    low_b = (b_base + 2 * bit0).astype(F32) * (1.0 / N_XLINE)
    prepare(unit_a, 2.0 / N_INLINE, low_b, 2.0 / N_XLINE)
    merge(
        0, 1, 2.0**-5, [(0, chosen(bit1 == 1))], (g0, g1, g2),
        [sign_of(full(0).astype(jnp.int32) + (b >> 1 & 1))],
        state_reader(wb_ref, 0), state_writer(wa_ref, lambda m: 0),
        lambda v: v + pltpu.roll(v, 2, 0),
    )
    g1 = g1 + sign_of(b >> 1 & 1) * 2.0**-5

    node_a = full(0.0) + a_base.astype(F32) * (1.0 / N_INLINE)
    prepare(node_a, 4.0 / N_INLINE, low_b, 2.0 / N_XLINE)
    even = bit0 == 0
    merge(
        1, 2, 2.0**-5, [(0, chosen(bit0 == 1))], (g0, g1, g2), [sign_of(bit1)],
        state_reader(wa_ref, 0), state_writer(wb_ref, lambda m: 0),
        lambda v: v + jnp.where(even, pltpu.roll(v, 7, 0), pltpu.roll(v, 1, 0)),
    )
    g2 = g2 + sign_of(bit1) * 2.0**-5

    node_b = full(0.0) + b_base.astype(F32) * (1.0 / N_XLINE)
    none = full(0).astype(jnp.int32)
    prepare(node_a, 4.0 / N_INLINE, node_b, 4.0 / N_XLINE)
    merge(
        0, 0, 2.0**-6, [(0, chosen(none + (a >> 2 & 1) == 1))], (g0, g1, g2), [sign_of(bit0)],
        state_reader(wb_ref, 0), state_writer(wa_ref, lambda m: 0), lambda v: v,
    )
    g0 = g0 + sign_of(bit0) * 2.0**-6

    node_a = full(0.0) + (a & ~7).astype(F32) * (1.0 / N_INLINE)
    prepare(node_a, 8.0 / N_INLINE, node_b, 4.0 / N_XLINE)
    merge(
        1, 1, 2.0**-6, [(0, chosen(none + (b >> 2 & 1) == 1))], (g0, g1, g2), [sign_of(bit2)],
        state_reader(wa_ref, 0), state_writer(wb_ref, lambda m: 0), lambda v: v,
    )
    g1 = g1 + sign_of(bit2) * 2.0**-6

    node_b = full(0.0) + (b & ~7).astype(F32) * (1.0 / N_XLINE)
    prepare(node_a, 8.0 / N_INLINE, node_b, 8.0 / N_XLINE)
    merge(
        0, 2, 2.0**-6, [(0, chosen(none + (a >> 3 & 1) == 1))], (g0, g1, g2), [-1.0, 1.0],
        state_reader(wb_ref, 0), state_writer(wa_ref, lambda m: m), lambda v: v,
    )

    node_a = full(0.0) + (a & ~15).astype(F32) * (1.0 / N_INLINE)
    prepare(node_a, 16.0 / N_INLINE, node_b, 8.0 / N_XLINE)
    mask = none + (b >> 3 & 1) == 1
    for k6 in range(2):
        merge(
            1, 0, 2.0**-7, [(0, chosen(mask))],
            (g0, g1, g2 + (2 * k6 - 1) * 2.0**-6), [-1.0, 1.0],
            state_reader(wa_ref, k6),
            (lambda k6: state_writer(wb_ref, lambda m: 2 * k6 + m))(k6), lambda v: v,
        )

    prepare(node_a, 16.0 / N_INLINE, full(0.0), 16.0 / N_XLINE)
    scale = 1.0 / math.sqrt(GC * NF * N_INLINE * N_XLINE)
    for k6 in range(2):
        for k7 in range(2):
            centre = (g0 + (2 * k7 - 1) * 2.0**-7, g1, g2 + (2 * k6 - 1) * 2.0**-6)
            anchor = 0.5 + centre[0]
            anchor_sq = anchor * anchor
            step = moves(centre, 1, 2.0**-7, [-1.0, 1.0])
            read = state_reader(wb_ref, 2 * k6 + k7)

            def body(b0, sums, anchor_sq=anchor_sq, centre=centre, step=step, read=read):
                sums = list(sums)
                for b1 in range(5):
                    w = [read(0, b0, b1, b2) for b2 in range(5)]
                    wp_re, wp_im = w[1][0] + w[3][0], w[1][1] + w[3][1]
                    wm_re, wm_im = w[1][0] - w[3][0], w[1][1] - w[3][1]
                    made = factors(anchor_sq, centre, 0, b0, b1, 1, step, 2.0**-7)
                    for m, (cu, su, cv, sv) in enumerate(made):
                        t_re, t_im = cmul(w[0][0], w[0][1], cu, su)
                        t_re = t_re + (w[2][0] + (cv * wp_re - sv * wm_im))
                        t_im = t_im + (w[2][1] + (cv * wp_im + sv * wm_re))
                        t_re, t_im = cmul(t_re, t_im, cu, su)
                        t_re, t_im = cmul(t_re + w[4][0], t_im + w[4][1], cu, su)
                        sums[2 * m] = sums[2 * m] + t_re
                        sums[2 * m + 1] = sums[2 * m + 1] + t_im
                return tuple(sums)

            sums = lax.fori_loop(0, 5, body, tuple(full(0.0) for _ in range(4)))
            for m in range(2):
                for part in range(2):
                    out_ref[pl.ds((2 * k6 + k7) * 32 + part * 2 + m, 8, stride=4), :] = (
                        sums[2 * m + part] * scale
                    )


def contributions(where, rows, interpret=False):
    return pl.pallas_call(
        kernel,
        out_shape=jax.ShapeDtypeStruct((128, 128), F32),
        in_specs=[
            pl.BlockSpec(memory_space=pltpu.SMEM),
            pl.BlockSpec(memory_space=pltpu.VMEM),
        ],
        out_specs=pl.BlockSpec(memory_space=pltpu.VMEM),
        scratch_shapes=[
            pltpu.VMEM((2, 2, 16, 8, 128), F32),
            pltpu.VMEM((23, 64, 128), F32),
            pltpu.VMEM((1280, 128), F32),
            pltpu.VMEM((2, 5, 8, 128), F32),
            pltpu.VMEM((2, 5, 8, 128), F32),
            pltpu.VMEM((2, 250, 8, 128), F32),
            pltpu.VMEM((4, 250, 8, 128), F32),
            pltpu.VMEM((200, 8, 128), F32),
        ],
        interpret=interpret,
    )(where, rows)


def shards(samples):
    rows = samples.reshape(1, 16, 128)
    rows = jnp.broadcast_to(rows, (16, 16, 128))
    rows = lax.all_to_all(rows, AXES, 0, 0, axis_index_groups=gather_groups())
    where = jnp.stack([lax.axis_index("inline"), lax.axis_index("xline")]).astype(jnp.int32)
    parts = contributions(where, rows).reshape(32, 4, 128)
    parts = lax.all_to_all(parts, AXES, 0, 0, axis_index_groups=scatter_groups())
    return jnp.sum(parts, axis=0).reshape(2, COLS)


def solution(mesh):
    return jax.shard_map(
        shards,
        mesh=mesh,
        in_specs=(P(None, "inline", "xline"),),
        out_specs=P(None, AXES),
        check_vma=False,
    )
```

```python
import math

import jax
import jax.numpy as jnp
import numpy as np
from jax import lax
from jax.experimental import pallas as pl
from jax.experimental.pallas import tpu as pltpu
from jax.sharding import PartitionSpec as P

NF = 256
COLS = 256
GC = 4
N_INLINE = 32
N_XLINE = 16
KAPPA = 40.0
AXES = ("inline", "xline")
F32 = jnp.float32
BF16 = jnp.bfloat16

ROOT = math.sqrt(0.5)
NODES = 0.5 * np.array([1.0, ROOT, 0.0, -ROOT, -1.0])


def basis_at(points):
    rows = []
    for k in range(5):
        factor = np.ones_like(points)
        for j in range(5):
            if j != k:
                factor = factor * (points - NODES[j]) / (NODES[k] - NODES[j])
        rows.append(factor)
    return np.stack(rows)


CHILD = [basis_at((t - 0.5) * 0.5 + 0.5 * NODES) for t in (0, 1)]
LEAF_XLINE = basis_at((np.arange(GC) + 0.5) / GC - 0.5)


def gather_groups():
    groups = []
    for base in range(N_INLINE * N_XLINE):
        a, b = base // N_XLINE, base % N_XLINE
        if a & 3 or b & 3:
            continue
        members = []
        for j in range(16):
            a0, b0, a1, b1 = j >> 3 & 1, j >> 2 & 1, j >> 1 & 1, j & 1
            members.append((a | a0 | a1 << 1) * N_XLINE + (b | b0 | b1 << 1))
        groups.append(members)
    return groups


def scatter_groups():
    groups = []
    for base in range(N_INLINE * N_XLINE):
        a, b = base // N_XLINE, base % N_XLINE
        if a >> 2 or b >> 2:
            continue
        members = []
        for j in range(32):
            k6, k7, k5, k3, k4 = j >> 4 & 1, j >> 3 & 1, j >> 2 & 1, j >> 1 & 1, j & 1
            members.append(
                (a | k3 << 2 | k5 << 3 | k7 << 4) * N_XLINE + (b | k4 << 2 | k6 << 3)
            )
        groups.append(members)
    return groups


def series(scale, bound, odd):
    coefs = []
    n = 0
    while True:
        power = 2 * n + (1 if odd else 0)
        size = (scale * bound) ** power / math.factorial(power)
        if size < 1e-8:
            return coefs
        coefs.append((-1.0) ** n * scale**power / math.factorial(power))
        n += 1


def poly(coefs, square):
    total = square * coefs[-1] + coefs[-2]
    for coef in coefs[-3::-1]:
        total = total * square + coef
    return total


def sincos_small(r, scale, bound):
    square = r * r
    return r * poly(series(scale, bound, True), square), poly(series(scale, bound, False), square)


def sincos_wide(x):
    turns = jnp.floor(x * (2.0 / math.pi) + 0.5)
    r = x - turns * 1.5703125
    r = r - turns * 4.837512969970703125e-4
    r = r - turns * 7.54978995489188216e-8
    sine, cosine = sincos_small(r, 1.0, 0.8)
    quarter = turns.astype(jnp.int32)
    swap = (quarter & 1) == 1
    s = jnp.where(swap, cosine, sine)
    c = jnp.where(swap, sine, cosine)
    s = jnp.where((quarter & 2) == 2, -s, s)
    c = jnp.where(((quarter + 1) & 2) == 2, -c, c)
    return s, c


def cmul(ar, ai, br, bi):
    return ar * br - ai * bi, ar * bi + ai * br


def full(value):
    return jnp.full((8, 128), value, F32)


def spot(bit):
    return (2 * bit - 1).astype(F32)


def places(where_ref):
    a = where_ref[0]
    b = where_ref[1]
    lane = lax.broadcasted_iota(jnp.int32, (8, 128), 1)
    sub = lax.broadcasted_iota(jnp.int32, (8, 128), 0)
    column = lane + ((a & 1) << 7)

    def digits(where):
        coord = full(0.5 * 0.5 ** len(where))
        for rank, place in enumerate(where):
            coord = coord + (column >> place & 1).astype(F32) * 0.5 ** (rank + 1)
        return coord

    return a, b, lane, sub, (digits((7, 4, 1)), digits((6, 3, 0)), digits((5, 2)))


def five(factor):
    c1, s1, cv, sv = factor
    c2 = c1 * c1 - s1 * s1
    s2 = c1 * s1
    s2 = s2 + s2
    c3, s3 = cmul(c2, s2, c1, s1)
    cc, ss, cs, sc = c2 * cv, s2 * sv, c2 * sv, s2 * cv
    return [(c3, s3), (cc - ss, sc + cs), (c2, s2), (cc + ss, sc - cs), (c1, s1)]


SETS = ((0, 1), (1, 2), (2, 3), (3, 4), (4, 5), (5, 7), (7, 11), (11, 19))
TURN = 40
NEAR = 11


def stretch(k, source, target, sem):
    low, high = SETS[k]
    at = pl.ds(low * 100, (high - low) * 100)
    return pltpu.make_async_copy(source.at[at], target.at[at], sem)


def table_kernel(where_ref, near_ref, turn_ref, far_ref, table_ref, tab_ref, far_s, table_s, p_ref, q_ref, s_ref, sems):
    a, b, lane, sub, (g0, g1, g2) = places(where_ref)
    bit2 = sub >> 2 & 1
    bit1 = sub >> 1 & 1
    bit0 = sub & 1
    none = sub * 0
    a_base = a & ~3
    b_base = b & ~3

    for half in range(2):
        box_a = (a_base + half + 2 * bit1).astype(F32)
        box_b = (b_base + bit2 + 2 * bit0).astype(F32)
        x0 = (box_a + 0.5) * (1.0 / N_INLINE)
        part = (0.5 + g0) * (0.5 + g0) + g1 * (x0 * x0)
        for c in range(GC):
            at = pl.ds(c * 16 + half * 8, 8)
            x1 = (box_b + (c + 0.5) / GC) * (1.0 / N_XLINE)
            radicand = part + g2 * (x1 * x1)
            step = (KAPPA / NF) * (radicand * lax.rsqrt(radicand))
            tab_ref[0, at, :] = step
            s, co = sincos_wide(step * 132.0)
            s64, c64 = sincos_wide(step * 64.0)
            for f1 in range(4):
                turn_ref[TURN + f1 * 16 + c * 2 + half] = co
                turn_ref[TURN + f1 * 16 + 8 + c * 2 + half] = s
                if f1 < 3:
                    co, s = cmul(co, s, c64, s64)
            s8, c8 = sincos_wide(step * 8.0)
            co, s = c8, s8
            for f2 in range(1, 8):
                tab_ref[2 * f2 - 1, at, :] = co
                tab_ref[2 * f2, at, :] = s
                if f2 < 7:
                    co, s = cmul(co, s, c8, s8)

    offset = sub.astype(F32) - 3.5

    def wave(box, ref, first):
        for c in range(GC):
            row = c * 16 + box

            def table(i):
                return jnp.broadcast_to(tab_ref[i, pl.ds(row, 1), :], (8, 128))

            s_a, c_a = sincos_small(table(0) * offset, 1.0, 1.15)
            cos_rows, sin_rows = [c_a], [s_a]
            for f2 in range(1, 8):
                cr, sr = cmul(c_a, s_a, table(2 * f2 - 1), table(2 * f2))
                cos_rows.append(cr)
                sin_rows.append(sr)
            right = jnp.concatenate(cos_rows + sin_rows, axis=0)
            right_hi = right.astype(BF16)
            ref[(box - first) * GC + c, 0:128, :] = right_hi
            ref[(box - first) * GC + c, 128:256, :] = (right - right_hi.astype(F32)).astype(BF16)

    def far_wave(box, carry):
        wave(box, far_s, NEAR)
        return carry

    def near_wave(box, carry):
        wave(box, near_ref, 0)
        return carry

    lax.fori_loop(NEAR, 16, far_wave, 0)
    save_far = pltpu.make_async_copy(far_s, far_ref, sems.at[8])
    save_far.start()

    def save(k):
        stretch(k, table_s, table_ref, sems.at[k]).start()

    def box_squares(low, width):
        return [(low + width * (float(NODES[k]) + 0.5)) * (low + width * (float(NODES[k]) + 0.5)) for k in range(5)]

    def level(low0, width0, low1, width1, centre, dim, q, sigmas, store, first=False):
        anchor = 0.5 + centre[0]
        x0 = box_squares(low0, width0)
        x1 = box_squares(low1, width1)
        for k in range(5):
            p_ref[k] = anchor * anchor + centre[1] * x0[k]
            q_ref[k] = centre[2] * x1[k]
            if dim:
                s_ref[k] = (x0 if dim == 1 else x1)[k] * q + full(0.0)
        if dim == 0:
            gaps = [2.0 * q * sigma * anchor + q * q for sigma in sigmas]

        def body(b1, carry):
            across = q_ref[b1]
            for b0 in (2,) if first else range(5):
                radicand = p_ref[b0] + across
                root = radicand * lax.rsqrt(radicand)
                for m, sigma in enumerate(sigmas):
                    if dim == 0:
                        moved = radicand + gaps[m]
                    else:
                        gap = s_ref[b0 if dim == 1 else b1]
                        if isinstance(sigma, float):
                            moved = radicand + gap if sigma > 0 else radicand - gap
                        else:
                            moved = radicand + sigma * gap
                    change = moved * lax.rsqrt(moved) - root
                    s_u, c_u = sincos_small(change, 0.5 * KAPPA, q)
                    s_v, c_v = sincos_small(change, KAPPA * float(NODES[1]), q)
                    store(m, b0, b1, (c_u, s_u, c_v, s_v))
            return carry

        lax.fori_loop(0, 5, body, 0)

    def into_levels(index_of):
        def store(m, b0, b1, factor):
            for k in range(4):
                table_s[index_of(m) * 100 + (b0 * 5 + b1) * 4 + k] = factor[k]

        return store

    unit_b = (b_base + bit2 + 2 * bit0).astype(F32) * (1.0 / N_XLINE)
    unit_a = (a_base + 2 * bit1).astype(F32) * (1.0 / N_INLINE)
    for side in range(2):

        def into_first(m, b0, b1, factor, side=side):
            for k in range(4):
                turn_ref[side * 20 + b1 * 4 + k] = factor[k]

        level(
            unit_a + side / N_INLINE, 1.0 / N_INLINE, unit_b, 1.0 / N_XLINE,
            (g0, g1, g2), 2, 2.0**-4, [spot(none + (b & 1))], into_first, True,
        )
    g2 = g2 + spot(none + (b & 1)) * 2.0**-4

    level(
        unit_a, 2.0 / N_INLINE, unit_b, 1.0 / N_XLINE,
        (g0, g1, g2), 0, 2.0**-5, [spot(none + (a >> 1 & 1))], into_levels(lambda m: 0),
    )
    save(0)
    g0 = g0 + spot(none + (a >> 1 & 1)) * 2.0**-5

    low_b = (b_base + 2 * bit0).astype(F32) * (1.0 / N_XLINE)
    level(
        unit_a, 2.0 / N_INLINE, low_b, 2.0 / N_XLINE,
        (g0, g1, g2), 1, 2.0**-5, [spot(none + (b >> 1 & 1))], into_levels(lambda m: 1),
    )
    save(1)
    g1 = g1 + spot(none + (b >> 1 & 1)) * 2.0**-5

    node_a = full(0.0) + a_base.astype(F32) * (1.0 / N_INLINE)
    level(
        node_a, 4.0 / N_INLINE, low_b, 2.0 / N_XLINE,
        (g0, g1, g2), 2, 2.0**-5, [spot(bit1)], into_levels(lambda m: 2),
    )
    save(2)
    g2 = g2 + spot(bit1) * 2.0**-5

    node_b = full(0.0) + b_base.astype(F32) * (1.0 / N_XLINE)
    level(
        node_a, 4.0 / N_INLINE, node_b, 4.0 / N_XLINE,
        (g0, g1, g2), 0, 2.0**-6, [spot(bit0)], into_levels(lambda m: 3),
    )
    save(3)
    g0 = g0 + spot(bit0) * 2.0**-6

    node_a = full(0.0) + (a & ~7).astype(F32) * (1.0 / N_INLINE)
    level(
        node_a, 8.0 / N_INLINE, node_b, 4.0 / N_XLINE,
        (g0, g1, g2), 1, 2.0**-6, [spot(bit2)], into_levels(lambda m: 4),
    )
    save(4)
    g1 = g1 + spot(bit2) * 2.0**-6

    node_b = full(0.0) + (b & ~7).astype(F32) * (1.0 / N_XLINE)
    level(
        node_a, 8.0 / N_INLINE, node_b, 8.0 / N_XLINE,
        (g0, g1, g2), 2, 2.0**-6, [-1.0, 1.0], into_levels(lambda m: 5 + m),
    )
    save(5)

    node_a = full(0.0) + (a & ~15).astype(F32) * (1.0 / N_INLINE)
    for k6 in range(2):
        level(
            node_a, 16.0 / N_INLINE, node_b, 8.0 / N_XLINE,
            (g0, g1, g2 + (2 * k6 - 1) * 2.0**-6), 0, 2.0**-7, [-1.0, 1.0],
            into_levels((lambda k6: lambda m: 7 + 2 * k6 + m)(k6)),
        )
    save(6)

    for k6 in range(2):
        for k7 in range(2):

            def into_last(m, b0, b1, factor, first=11 + 4 * k6 + 2 * k7):
                for k in range(4):
                    table_s[(first + m) * 100 + (b0 * 5 + b1) * 4 + k] = factor[k]

            level(
                node_a, 16.0 / N_INLINE, full(0.0), 16.0 / N_XLINE,
                (g0 + (2 * k7 - 1) * 2.0**-7, g1, g2 + (2 * k6 - 1) * 2.0**-6), 1, 2.0**-7,
                [-1.0, 1.0], into_last,
            )
    save(7)
    lax.fori_loop(0, NEAR, near_wave, 0)
    save_far.wait()
    for k in range(8):
        stretch(k, table_s, table_ref, sems.at[k]).wait()


def kernel(where_ref, rows_ref, near_ref, turn_ref, far_ref, table_ref, out_ref, v_ref, leaf_ref, wa_ref, wb_ref, x_ref, far_s, table_s, sems):
    load_far = pltpu.make_async_copy(far_ref, far_s, sems.at[8])
    load_far.start()
    loads = [stretch(k, table_ref, table_s, sems.at[k]) for k in range(8)]
    for load in loads:
        load.start()
    a, b, lane, sub, unused = places(where_ref)

    left = lax.broadcasted_iota(jnp.int32, (16, 8, 128), 2) < 64
    re = rows_ref[:, 0:8, :]
    im = rows_ref[:, 8:16, :]
    re_r = pltpu.roll(re, 64, 2)
    im_r = pltpu.roll(im, 64, 2)
    v_ref[0, 0] = jnp.where(left, re, -im_r)
    v_ref[1, 0] = jnp.where(left, re_r, -im)
    v_ref[0, 1] = jnp.where(left, im, re_r)
    v_ref[1, 1] = jnp.where(left, im_r, re)

    basis = []
    for f1 in range(4):
        z = ((lane & 63).astype(F32) + (f1 * 64 + 0.5)) * (1.0 / NF) - 0.5
        factor = jnp.zeros((8, 128), F32)
        for k in range(5):
            scale = 1.0
            for j in range(5):
                if j != k:
                    scale = scale / (NODES[k] - NODES[j])
            factor = jnp.where(sub == k, scale, factor)
        for j in range(5):
            factor = factor * jnp.where(sub == j, 1.0, z - NODES[j])
        basis.append(factor)

    def leaf_one(box):
        totals = []
        for c in range(GC):
            def table(i):
                return jnp.broadcast_to(turn_ref[TURN + i * 8 + c * 2 + box // 8, pl.ds(box % 8, 1), :], (8, 128))

            rows = []
            for f1 in range(4):
                for part in range(2):
                    sample = v_ref[f1 & 1, part, pl.ds(box, 1), 2 * c + f1 // 2, :]
                    rows.append(basis[f1] * jnp.broadcast_to(sample, (8, 128)))
            lhs = jnp.concatenate(rows, axis=0)
            lhs_hi = lhs.astype(BF16)
            lhs_lo = (lhs - lhs_hi.astype(F32)).astype(BF16)
            both = jnp.concatenate([lhs_hi, lhs_hi], axis=1)
            right = near_ref[box * GC + c] if box < NEAR else far_s[(box - NEAR) * GC + c]
            mixed = jnp.dot(both, right, preferred_element_type=F32)
            mixed = mixed + jnp.dot(lhs_lo, right[0:128], preferred_element_type=F32)
            t_re = None
            for f1 in range(4):
                u_re = mixed[f1 * 16 : f1 * 16 + 8]
                u_im = mixed[f1 * 16 + 8 : f1 * 16 + 16]
                r_re, r_im = cmul(u_re, u_im, table(2 * f1), table(2 * f1 + 1))
                t_re, t_im = (r_re, r_im) if t_re is None else (t_re + r_re, t_im + r_im)
            totals.append((t_re, t_im))
        for a1 in range(5):
            for part in range(2):
                total = totals[0][part] * float(LEAF_XLINE[a1, 0])
                for c in range(1, GC):
                    total = total + totals[c][part] * float(LEAF_XLINE[a1, c])
                leaf_ref[pl.ds((a1 * 16 + part) * 16 + box, 8, stride=32), :] = total

    for box in range(16):
        if box == NEAR:
            load_far.wait()
        leaf_one(box)

    def merge(axis, points, sets, read, turn, weight, write, combine):
        def body(other, carry):
            for n, (side, p) in enumerate(points):
                b0, b1 = (p, other) if axis == 0 else (other, p)
                turns = [five(turn(m, side, b0, b1)) for m in range(sets)]
                for b2 in range(5):
                    w_re, w_im = read(side, b0, b1, b2)
                    for m in range(sets):
                        x_re, x_im = cmul(w_re, w_im, *turns[m][b2])
                        x_ref[(m * 5 + n) * 10 + 2 * b2] = x_re
                        x_ref[(m * 5 + n) * 10 + 2 * b2 + 1] = x_im
            for m in range(sets):
                for comp in range(10):
                    items = [x_ref[(m * 5 + n) * 10 + comp] for n in range(len(points))]
                    for i in range(5):
                        total = None
                        for (side, p), item in zip(points, items):
                            coef = weight(i, side, p)
                            if coef is None:
                                continue
                            term = item if isinstance(coef, float) and coef == 1.0 else item * coef
                            total = term if total is None else total + term
                        i0, i1 = (i, other) if axis == 0 else (other, i)
                        write(m, i0, i1, comp, combine(total))
            return carry

        lax.fori_loop(0, 5, body, 0)

    def chosen(mask):
        table = [
            [
                None
                if CHILD[0][i, j] == 0.0 and CHILD[1][i, j] == 0.0
                else jnp.where(mask, float(CHILD[1][i, j]), float(CHILD[0][i, j]))
                for j in range(5)
            ]
            for i in range(5)
        ]
        return lambda i, side, j: table[i][j]

    def lower(i, side, j):
        return None if CHILD[0][i, j] == 0.0 else float(CHILD[0][i, j])

    def flipped(axis, bit):
        def order(i0, i1):
            if axis == 0:
                return i0 + bit * (4 - 2 * i0), i1
            return i0, i1 + bit * (4 - 2 * i1)

        return order

    def same(i0, i1):
        return i0, i1

    def reader(ref, index, order=same):
        def read(side, b0, b1, b2):
            b0, b1 = order(b0, b1)
            at = (b0 * 5 + b1) * 10 + b2 * 2
            return ref[index, at], ref[index, at + 1]

        return read

    def turner(index_of, order=same):
        def turn(m, side, b0, b1):
            b0, b1 = order(b0, b1)
            at = index_of(m) * 100 + (b0 * 5 + b1) * 4
            return [table_s[at + k] for k in range(4)]

        return turn

    def writer(ref, index_of, order=same):
        def write(m, i0, i1, comp, value):
            i0, i1 = order(i0, i1)
            ref[index_of(m), (i0 * 5 + i1) * 10 + comp] = value

        return write

    line = [(0, j) for j in range(5)]

    def leaf_read(side, b0, b1, b2):
        base = pl.multiple_of((b1 * 8 + b2) * 32 + side * 8, 8)
        return leaf_ref[pl.ds(base, 8), :], leaf_ref[pl.ds(base + 16, 8), :]

    merge(
        0, [(0, 2), (1, 2)], 1, leaf_read,
        lambda m, side, b0, b1: [turn_ref[side * 20 + b1 * 4 + k] for k in range(4)],
        lambda i, side, j: float(CHILD[side][i, j]),
        writer(wa_ref, lambda m: 0), lambda v: v,
    )
    loads[0].wait()
    merge(
        1, line, 1, reader(wa_ref, 0), turner(lambda m: 0), chosen((sub >> 2 & 1) == 1),
        writer(wb_ref, lambda m: 0), lambda v: v + pltpu.roll(v, 4, 0),
    )
    loads[1].wait()
    merge(
        0, line, 1, reader(wb_ref, 0), turner(lambda m: 1), chosen((sub >> 1 & 1) == 1),
        writer(wa_ref, lambda m: 0), lambda v: v + pltpu.roll(v, 2, 0),
    )
    loads[2].wait()
    even = (sub & 1) == 0
    merge(
        1, line, 1, reader(wa_ref, 0), turner(lambda m: 2), chosen((sub & 1) == 1),
        writer(wb_ref, lambda m: 0),
        lambda v: v + jnp.where(even, pltpu.roll(v, 7, 0), pltpu.roll(v, 1, 0)),
    )
    loads[3].wait()
    order = flipped(0, a >> 2 & 1)
    merge(
        0, line, 1, reader(wb_ref, 0, order), turner(lambda m: 3, order), lower,
        writer(wa_ref, lambda m: 0, order), lambda v: v,
    )
    loads[4].wait()
    order = flipped(1, b >> 2 & 1)
    merge(
        1, line, 1, reader(wa_ref, 0, order), turner(lambda m: 4, order), lower,
        writer(wb_ref, lambda m: 0, order), lambda v: v,
    )
    loads[5].wait()
    order = flipped(0, a >> 3 & 1)
    merge(
        0, line, 2, reader(wb_ref, 0, order), turner(lambda m: 5 + m, order), lower,
        writer(wa_ref, lambda m: m, order), lambda v: v,
    )
    loads[6].wait()
    order = flipped(1, b >> 3 & 1)
    for k6 in range(2):
        merge(
            1, line, 2, reader(wa_ref, k6, order),
            turner((lambda k6: lambda m: 7 + 2 * k6 + m)(k6), order), lower,
            writer(wb_ref, (lambda k6: lambda m: 2 * k6 + m)(k6), order), lambda v: v,
        )

    loads[7].wait()
    scale = 1.0 / math.sqrt(GC * NF * N_INLINE * N_XLINE)
    for k67 in range(4):
        read = reader(wb_ref, k67)

        def body(b0, sums, k67=k67, read=read):
            sums = list(sums)
            for b1 in range(5):
                w = [read(0, b0, b1, b2) for b2 in range(5)]
                wp_re, wp_im = w[1][0] + w[3][0], w[1][1] + w[3][1]
                wm_re, wm_im = w[1][0] - w[3][0], w[1][1] - w[3][1]
                for m in range(2):
                    cu, su, cv, sv = (table_s[(11 + 2 * k67 + m) * 100 + (b0 * 5 + b1) * 4 + k] for k in range(4))
                    t_re, t_im = cmul(w[0][0], w[0][1], cu, su)
                    t_re = t_re + (w[2][0] + (cv * wp_re - sv * wm_im))
                    t_im = t_im + (w[2][1] + (cv * wp_im + sv * wm_re))
                    t_re, t_im = cmul(t_re, t_im, cu, su)
                    t_re, t_im = cmul(t_re + w[4][0], t_im + w[4][1], cu, su)
                    sums[2 * m] = sums[2 * m] + t_re
                    sums[2 * m + 1] = sums[2 * m + 1] + t_im
            return tuple(sums)

        sums = lax.fori_loop(0, 5, body, tuple(full(0.0) for _ in range(4)))
        for m in range(2):
            for part in range(2):
                out_ref[pl.ds(k67 * 32 + part * 2 + m, 8, stride=4), :] = sums[2 * m + part] * scale


def in_vmem():
    return pl.BlockSpec(memory_space=pltpu.VMEM)


def in_hbm():
    return pl.BlockSpec(memory_space=pltpu.HBM)


def tables(where, interpret=False):
    return pl.pallas_call(
        table_kernel,
        out_shape=[
            jax.ShapeDtypeStruct((NEAR * GC, 256, 128), BF16),
            jax.ShapeDtypeStruct((TURN + 64, 8, 128), F32),
            pltpu.HBM(((16 - NEAR) * GC, 256, 128), BF16),
            pltpu.HBM((1900, 8, 128), F32),
        ],
        in_specs=[pl.BlockSpec(memory_space=pltpu.SMEM)],
        out_specs=[in_vmem(), in_vmem(), in_hbm(), in_hbm()],
        scratch_shapes=[
            pltpu.VMEM((15, 64, 128), F32),
            pltpu.VMEM(((16 - NEAR) * GC, 256, 128), BF16),
            pltpu.VMEM((1900, 8, 128), F32),
            pltpu.VMEM((5, 8, 128), F32),
            pltpu.VMEM((5, 8, 128), F32),
            pltpu.VMEM((5, 8, 128), F32),
            pltpu.SemaphoreType.DMA((9,)),
        ],
        compiler_params=pltpu.CompilerParams(vmem_limit_bytes=14 << 20),
        interpret=interpret,
    )(where)


def contributions(where, rows, interpret=False):
    near, turn, far, table = tables(where, interpret)
    if not interpret:
        far = pltpu.with_memory_space_constraint(far, pltpu.HBM)
        table = pltpu.with_memory_space_constraint(table, pltpu.HBM)
    return pl.pallas_call(
        kernel,
        out_shape=jax.ShapeDtypeStruct((128, 128), F32),
        in_specs=[pl.BlockSpec(memory_space=pltpu.SMEM), in_vmem(), in_vmem(), in_vmem(), in_hbm(), in_hbm()],
        out_specs=in_vmem(),
        scratch_shapes=[
            pltpu.VMEM((2, 2, 16, 8, 128), F32),
            pltpu.VMEM((1280, 128), F32),
            pltpu.VMEM((2, 250, 8, 128), F32),
            pltpu.VMEM((4, 250, 8, 128), F32),
            pltpu.VMEM((100, 8, 128), F32),
            pltpu.VMEM(((16 - NEAR) * GC, 256, 128), BF16),
            pltpu.VMEM((1900, 8, 128), F32),
            pltpu.SemaphoreType.DMA((9,)),
        ],
        compiler_params=pltpu.CompilerParams(vmem_limit_bytes=20 << 20),
        interpret=interpret,
    )(where, rows, near, turn, far, table)


def shards(samples):
    rows = samples.reshape(1, 16, 128)
    rows = jnp.broadcast_to(rows, (16, 16, 128))
    rows = lax.all_to_all(rows, AXES, 0, 0, axis_index_groups=gather_groups())
    where = jnp.stack([lax.axis_index("inline"), lax.axis_index("xline")]).astype(jnp.int32)
    parts = contributions(where, rows).reshape(32, 4, 128)
    parts = lax.all_to_all(parts, AXES, 0, 0, axis_index_groups=scatter_groups())
    return jnp.sum(parts, axis=0).reshape(2, COLS)


def solution(mesh):
    return jax.shard_map(
        shards,
        mesh=mesh,
        in_specs=(P(None, "inline", "xline"),),
        out_specs=P(None, AXES),
        check_vma=False,
    )
```

```python
import functools
import math

import jax
import jax.numpy as jnp
import numpy as np
from jax import lax
from jax.experimental import pallas as pl
from jax.experimental.pallas import tpu as pltpu
from jax.sharding import PartitionSpec as P

NF = 256
COLS = 256
GC = 4
N_INLINE = 32
N_XLINE = 16
KAPPA = 40.0
AXES = ("inline", "xline")
F32 = jnp.float32
BF16 = jnp.bfloat16

ROOT = math.sqrt(0.5)
NODES = 0.5 * np.array([1.0, ROOT, 0.0, -ROOT, -1.0])


def basis_at(points):
    rows = []
    for k in range(5):
        factor = np.ones_like(points)
        for j in range(5):
            if j != k:
                factor = factor * (points - NODES[j]) / (NODES[k] - NODES[j])
        rows.append(factor)
    return np.stack(rows)


CHILD = [basis_at((t - 0.5) * 0.5 + 0.5 * NODES) for t in (0, 1)]
LEAF_XLINE = basis_at((np.arange(GC) + 0.5) / GC - 0.5)


def gather_groups():
    groups = []
    for base in range(N_INLINE * N_XLINE):
        a, b = base // N_XLINE, base % N_XLINE
        if a & 3 or b & 3:
            continue
        members = []
        for j in range(16):
            a0, b0, a1, b1 = j >> 3 & 1, j >> 2 & 1, j >> 1 & 1, j & 1
            members.append((a | a0 | a1 << 1) * N_XLINE + (b | b0 | b1 << 1))
        groups.append(members)
    return groups


def scatter_groups():
    groups = []
    for base in range(N_INLINE * N_XLINE):
        a, b = base // N_XLINE, base % N_XLINE
        if a >> 2 or b >> 2:
            continue
        members = []
        for j in range(32):
            k6, k7, k5, k3, k4 = j >> 4 & 1, j >> 3 & 1, j >> 2 & 1, j >> 1 & 1, j & 1
            members.append(
                (a | k3 << 2 | k5 << 3 | k7 << 4) * N_XLINE + (b | k4 << 2 | k6 << 3)
            )
        groups.append(members)
    return groups


def series(scale, bound, odd):
    coefs = []
    n = 0
    while True:
        power = 2 * n + (1 if odd else 0)
        size = (scale * bound) ** power / math.factorial(power)
        if size < 3e-8:
            return coefs
        coefs.append((-1.0) ** n * scale**power / math.factorial(power))
        n += 1


def poly(coefs, square):
    total = square * coefs[-1] + coefs[-2]
    for coef in coefs[-3::-1]:
        total = total * square + coef
    return total


def sincos_small(r, scale, bound):
    square = r * r
    return r * poly(series(scale, bound, True), square), poly(series(scale, bound, False), square)


def sincos_wide(x):
    turns = jnp.floor(x * (2.0 / math.pi) + 0.5)
    r = x - turns * 1.5703125
    r = r - turns * 4.837512969970703125e-4
    r = r - turns * 7.54978995489188216e-8
    sine, cosine = sincos_small(r, 1.0, 0.8)
    quarter = turns.astype(jnp.int32)
    swap = (quarter & 1) == 1
    s = jnp.where(swap, cosine, sine)
    c = jnp.where(swap, sine, cosine)
    s = jnp.where((quarter & 2) == 2, -s, s)
    c = jnp.where(((quarter + 1) & 2) == 2, -c, c)
    return s, c


def cmul(ar, ai, br, bi):
    return ar * br - ai * bi, ar * bi + ai * br


def full(value):
    return jnp.full((8, 128), value, F32)


def spot(bit):
    return (2 * bit - 1).astype(F32)


def places(where):
    a, b = where()
    lane = lax.broadcasted_iota(jnp.int32, (8, 128), 1)
    sub = lax.broadcasted_iota(jnp.int32, (8, 128), 0)
    column = lane + ((a & 1) << 7)

    def digits(where):
        coord = full(0.5 * 0.5 ** len(where))
        for rank, place in enumerate(where):
            coord = coord + (column >> place & 1).astype(F32) * 0.5 ** (rank + 1)
        return coord

    return a, b, lane, sub, (digits((7, 4, 1)), digits((6, 3, 0)), digits((5, 2)))


def five(factor):
    c1, s1, cv, sv = factor
    c2 = c1 * c1 - s1 * s1
    s2 = c1 * s1
    s2 = s2 + s2
    c3, s3 = cmul(c2, s2, c1, s1)
    cc, ss, cs, sc = c2 * cv, s2 * sv, c2 * sv, s2 * cv
    return [(c3, s3), (cc - ss, sc + cs), (c2, s2), (cc + ss, sc - cs), (c1, s1)]


NEAR = 11
STRETCHES = ((7, 11), (11, 15), (15, 19))


def stretch(k, table, held, sem, out):
    low, high = STRETCHES[k]
    far = table.at[pl.ds((low - 7) * 100, (high - low) * 100)]
    near = held.at[pl.ds(low * 100, (high - low) * 100)]
    return pltpu.make_async_copy(near, far, sem) if out else pltpu.make_async_copy(far, near, sem)


def plan(a, b, sub, centre):
    g0, g1, g2 = centre
    bit2, bit1, bit0, none = sub >> 2 & 1, sub >> 1 & 1, sub & 1, sub * 0
    a_base = a & ~3
    b_base = b & ~3
    unit_b = (b_base + bit2 + 2 * bit0).astype(F32) * (1.0 / N_XLINE)
    unit_a = (a_base + 2 * bit1).astype(F32) * (1.0 / N_INLINE)
    low_b = (b_base + 2 * bit0).astype(F32) * (1.0 / N_XLINE)

    def inline_low(bits):
        return (none + (a >> bits << bits)).astype(F32) * (1.0 / N_INLINE)

    def xline_low(bits):
        return (none + (b >> bits << bits)).astype(F32) * (1.0 / N_XLINE)

    levels = []
    sign = spot(none + (b & 1))
    for side in range(2):
        box = (unit_a + side / N_INLINE, 1.0 / N_INLINE, unit_b, 1.0 / N_XLINE)
        levels.append((box, (g0, g1, g2), 2, 2.0**-4, [sign], side))
    g2 = g2 + sign * 2.0**-4
    sign = spot(none + (a >> 1 & 1))
    box = (unit_a, 2.0 / N_INLINE, unit_b, 1.0 / N_XLINE)
    levels.append((box, (g0, g1, g2), 0, 2.0**-5, [sign], 0))
    g0 = g0 + sign * 2.0**-5
    sign = spot(none + (b >> 1 & 1))
    box = (unit_a, 2.0 / N_INLINE, low_b, 2.0 / N_XLINE)
    levels.append((box, (g0, g1, g2), 1, 2.0**-5, [sign], 1))
    g1 = g1 + sign * 2.0**-5
    sign = spot(bit1)
    box = (inline_low(2), 4.0 / N_INLINE, low_b, 2.0 / N_XLINE)
    levels.append((box, (g0, g1, g2), 2, 2.0**-5, [sign], 2))
    g2 = g2 + sign * 2.0**-5
    sign = spot(bit0)
    box = (inline_low(2), 4.0 / N_INLINE, xline_low(2), 4.0 / N_XLINE)
    levels.append((box, (g0, g1, g2), 0, 2.0**-6, [sign], 3))
    g0 = g0 + sign * 2.0**-6
    sign = spot(bit2)
    box = (inline_low(3), 8.0 / N_INLINE, xline_low(2), 4.0 / N_XLINE)
    levels.append((box, (g0, g1, g2), 1, 2.0**-6, [sign], 4))
    g1 = g1 + sign * 2.0**-6
    box = (inline_low(3), 8.0 / N_INLINE, xline_low(3), 8.0 / N_XLINE)
    levels.append((box, (g0, g1, g2), 2, 2.0**-6, [-1.0, 1.0], 5))
    for k6 in range(2):
        box = (inline_low(4), 16.0 / N_INLINE, xline_low(3), 8.0 / N_XLINE)
        centre = (g0, g1, g2 + (2 * k6 - 1) * 2.0**-6)
        levels.append((box, centre, 0, 2.0**-7, [-1.0, 1.0], 7 + 2 * k6))
    for k6 in range(2):
        for k7 in range(2):
            box = (inline_low(4), 16.0 / N_INLINE, full(0.0), 16.0 / N_XLINE)
            centre = (g0 + (2 * k7 - 1) * 2.0**-7, g1, g2 + (2 * k6 - 1) * 2.0**-6)
            levels.append((box, centre, 1, 2.0**-7, [-1.0, 1.0], 11 + 4 * k6 + 2 * k7))
    return levels


def turning(level, slot, p_ref, q_ref, s_ref, store):
    (low0, width0, low1, width1), centre, dim, q, signs, first = level
    anchor = 0.5 + centre[0]
    for k in range(5):
        place = float(NODES[k]) + 0.5
        x0 = (low0 + width0 * place) * (low0 + width0 * place)
        x1 = (low1 + width1 * place) * (low1 + width1 * place)
        p_ref[slot, k] = anchor * anchor + centre[1] * x0
        q_ref[slot, k] = centre[2] * x1
        if dim:
            s_ref[slot, k] = (x0 if dim == 1 else x1) * q
    for m, sign in enumerate(signs):
        if dim == 0:
            s_ref[slot, m] = 2.0 * q * sign * anchor + q * q

    def point(b0, b1):
        radicand = p_ref[slot, b0] + q_ref[slot, b1]
        root = radicand * lax.rsqrt(radicand)
        for m, sign in enumerate(signs):
            if dim == 0:
                moved = radicand + s_ref[slot, m]
            else:
                gap = s_ref[slot, b0 if dim == 1 else b1]
                if isinstance(sign, float):
                    moved = radicand + gap if sign > 0 else radicand - gap
                else:
                    moved = radicand + sign * gap
            change = moved * lax.rsqrt(moved) - root
            s_u, c_u = sincos_small(change, 0.5 * KAPPA, q)
            s_v, c_v = sincos_small(change, KAPPA * float(NODES[1]), q)
            store(first + m, b0, b1, (c_u, s_u, c_v, s_v))

    return point


def table_kernel(where, near_ref, turn_ref, far_ref, table_ref, tab_ref, far_s, table_s, p_ref, q_ref, s_ref, sems):
    a, b, lane, sub, (g0, g1, g2) = places(where)
    bit2 = sub >> 2 & 1
    bit1 = sub >> 1 & 1
    bit0 = sub & 1
    a_base = a & ~3
    b_base = b & ~3

    for half in range(2):
        box_a = (a_base + half + 2 * bit1).astype(F32)
        box_b = (b_base + bit2 + 2 * bit0).astype(F32)
        x0 = (box_a + 0.5) * (1.0 / N_INLINE)
        part = (0.5 + g0) * (0.5 + g0) + g1 * (x0 * x0)
        for c in range(GC):
            at = pl.ds(c * 16 + half * 8, 8)
            x1 = (box_b + (c + 0.5) / GC) * (1.0 / N_XLINE)
            radicand = part + g2 * (x1 * x1)
            step = (KAPPA / NF) * (radicand * lax.rsqrt(radicand))
            tab_ref[0, at, :] = step
            s, co = sincos_wide(step * 132.0)
            s64, c64 = sincos_wide(step * 64.0)
            for f1 in range(4):
                turn_ref[f1 * 16 + c * 2 + half] = co
                turn_ref[f1 * 16 + 8 + c * 2 + half] = s
                if f1 < 3:
                    co, s = cmul(co, s, c64, s64)
            s8, c8 = sincos_wide(step * 8.0)
            co, s = c8, s8
            for f2 in range(1, 8):
                tab_ref[2 * f2 - 1, at, :] = co
                tab_ref[2 * f2, at, :] = s
                if f2 < 7:
                    co, s = cmul(co, s, c8, s8)

    offset = sub.astype(F32) - 3.5

    def wave(box, ref, first):
        for c in range(GC):
            row = c * 16 + box

            def table(i):
                return jnp.broadcast_to(tab_ref[i, pl.ds(row, 1), :], (8, 128))

            s_a, c_a = sincos_small(table(0) * offset, 1.0, 1.15)
            cos_rows, sin_rows = [c_a], [s_a]
            for f2 in range(1, 8):
                cr, sr = cmul(c_a, s_a, table(2 * f2 - 1), table(2 * f2))
                cos_rows.append(cr)
                sin_rows.append(sr)
            right = jnp.concatenate(cos_rows + sin_rows, axis=0)
            right_hi = right.astype(BF16)
            ref[(box - first) * GC + c, 0:128, :] = right_hi
            ref[(box - first) * GC + c, 128:256, :] = (right - right_hi.astype(F32)).astype(BF16)

    def far_wave(box, carry):
        wave(box, far_s, NEAR)
        return carry

    def near_wave(box, carry):
        wave(box, near_ref, 0)
        return carry

    lax.fori_loop(NEAR, 16, far_wave, 0)
    save_far = pltpu.make_async_copy(far_s, far_ref, sems.at[3])
    save_far.start()

    def held(index, b0, b1, factor):
        for k in range(4):
            table_s[index * 100 + (b0 * 5 + b1) * 4 + k] = factor[k]

    saves = []
    for i, level in enumerate(plan(a, b, sub, (g0, g1, g2))[8:]):
        point = turning(level, 0, p_ref, q_ref, s_ref, held)

        def across(b1, carry, point=point):
            for b0 in range(5):
                point(b0, b1)
            return carry

        lax.fori_loop(0, 5, across, 0)
        if i % 2:
            k = i // 2
            saves.append(stretch(k, table_ref, table_s, sems.at[k], True))
            saves[-1].start()
    lax.fori_loop(0, NEAR, near_wave, 0)
    save_far.wait()
    for copy in saves:
        copy.wait()


def kernel(where, rows_ref, near_ref, turn_ref, far_ref, table_ref, out_ref, v_ref, leaf_ref, wa_ref, wb_ref, x_ref, far_s, table_s, first_s, p_ref, q_ref, s_ref, sems):
    load_far = pltpu.make_async_copy(far_ref, far_s, sems.at[3])
    load_far.start()
    loads = [stretch(k, table_ref, table_s, sems.at[k], False) for k in range(3)]
    for load in loads:
        load.start()
    a, b, lane, sub, kept = places(where)

    def hold_first(side, b0, b1, factor):
        for k in range(4):
            first_s[side * 20 + b1 * 4 + k] = factor[k]

    def hold(index, b0, b1, factor):
        for k in range(4):
            table_s[index * 100 + (b0 * 5 + b1) * 4 + k] = factor[k]

    points = []
    for i, level in enumerate(plan(a, b, sub, kept)[:8]):
        point = turning(level, i, p_ref, q_ref, s_ref, hold_first if i < 2 else hold)
        points += [(point, b0, b1) for b0 in ((2,) if i < 2 else range(5)) for b1 in range(5)]

    left = lax.broadcasted_iota(jnp.int32, (16, 8, 128), 2) < 64
    re = rows_ref[:, 0:8, :]
    im = rows_ref[:, 8:16, :]
    re_r = pltpu.roll(re, 64, 2)
    im_r = pltpu.roll(im, 64, 2)
    v_ref[0, 0] = jnp.where(left, re, -im_r)
    v_ref[1, 0] = jnp.where(left, re_r, -im)
    v_ref[0, 1] = jnp.where(left, im, re_r)
    v_ref[1, 1] = jnp.where(left, im_r, re)

    basis = []
    for f1 in range(4):
        z = ((lane & 63).astype(F32) + (f1 * 64 + 0.5)) * (1.0 / NF) - 0.5
        factor = jnp.zeros((8, 128), F32)
        for k in range(5):
            scale = 1.0
            for j in range(5):
                if j != k:
                    scale = scale / (NODES[k] - NODES[j])
            factor = jnp.where(sub == k, scale, factor)
        for j in range(5):
            factor = factor * jnp.where(sub == j, 1.0, z - NODES[j])
        basis.append(factor)

    def leaf_one(box):
        totals = []
        for c in range(GC):
            def table(i):
                return jnp.broadcast_to(turn_ref[i * 8 + c * 2 + box // 8, pl.ds(box % 8, 1), :], (8, 128))

            rows = []
            for f1 in range(4):
                for part in range(2):
                    sample = v_ref[f1 & 1, part, pl.ds(box, 1), 2 * c + f1 // 2, :]
                    rows.append(basis[f1] * jnp.broadcast_to(sample, (8, 128)))
            lhs = jnp.concatenate(rows, axis=0)
            lhs_hi = lhs.astype(BF16)
            lhs_lo = (lhs - lhs_hi.astype(F32)).astype(BF16)
            both = jnp.concatenate([lhs_hi, lhs_hi], axis=1)
            right = near_ref[box * GC + c] if box < NEAR else far_s[(box - NEAR) * GC + c]
            mixed = jnp.dot(both, right, preferred_element_type=F32)
            mixed = mixed + jnp.dot(lhs_lo, right[0:128], preferred_element_type=F32)
            t_re = None
            for f1 in range(4):
                u_re = mixed[f1 * 16 : f1 * 16 + 8]
                u_im = mixed[f1 * 16 + 8 : f1 * 16 + 16]
                r_re, r_im = cmul(u_re, u_im, table(2 * f1), table(2 * f1 + 1))
                t_re, t_im = (r_re, r_im) if t_re is None else (t_re + r_re, t_im + r_im)
            totals.append((t_re, t_im))
        for a1 in range(5):
            for part in range(2):
                total = totals[0][part] * float(LEAF_XLINE[a1, 0])
                for c in range(1, GC):
                    total = total + totals[c][part] * float(LEAF_XLINE[a1, c])
                leaf_ref[pl.ds((a1 * 16 + part) * 16 + box, 8, stride=32), :] = total

    for box in range(16):
        if box == NEAR:
            load_far.wait()
        leaf_one(box)
        for point, b0, b1 in points[box::16]:
            point(b0, b1)

    def merge(axis, points, sets, read, turn, weight, write, combine):
        def body(other, carry):
            for n, (side, p) in enumerate(points):
                b0, b1 = (p, other) if axis == 0 else (other, p)
                turns = [five(turn(m, side, b0, b1)) for m in range(sets)]
                for b2 in range(5):
                    w_re, w_im = read(side, b0, b1, b2)
                    for m in range(sets):
                        x_re, x_im = cmul(w_re, w_im, *turns[m][b2])
                        x_ref[(m * 5 + n) * 10 + 2 * b2] = x_re
                        x_ref[(m * 5 + n) * 10 + 2 * b2 + 1] = x_im
            for m in range(sets):
                for comp in range(10):
                    items = [x_ref[(m * 5 + n) * 10 + comp] for n in range(len(points))]
                    for i in range(5):
                        total = None
                        for (side, p), item in zip(points, items):
                            coef = weight(i, side, p)
                            if coef is None:
                                continue
                            term = item if isinstance(coef, float) and coef == 1.0 else item * coef
                            total = term if total is None else total + term
                        i0, i1 = (i, other) if axis == 0 else (other, i)
                        write(m, i0, i1, comp, combine(total))
            return carry

        lax.fori_loop(0, 5, body, 0)

    def chosen(mask):
        table = [
            [
                None
                if CHILD[0][i, j] == 0.0 and CHILD[1][i, j] == 0.0
                else jnp.where(mask, float(CHILD[1][i, j]), float(CHILD[0][i, j]))
                for j in range(5)
            ]
            for i in range(5)
        ]
        return lambda i, side, j: table[i][j]

    def lower(i, side, j):
        return None if CHILD[0][i, j] == 0.0 else float(CHILD[0][i, j])

    def flipped(axis, bit):
        def order(i0, i1):
            if axis == 0:
                return i0 + bit * (4 - 2 * i0), i1
            return i0, i1 + bit * (4 - 2 * i1)

        return order

    def same(i0, i1):
        return i0, i1

    def reader(ref, index, order=same):
        def read(side, b0, b1, b2):
            b0, b1 = order(b0, b1)
            at = (b0 * 5 + b1) * 10 + b2 * 2
            return ref[index, at], ref[index, at + 1]

        return read

    def turner(index_of, order=same):
        def turn(m, side, b0, b1):
            b0, b1 = order(b0, b1)
            at = index_of(m) * 100 + (b0 * 5 + b1) * 4
            return [table_s[at + k] for k in range(4)]

        return turn

    def writer(ref, index_of, order=same):
        def write(m, i0, i1, comp, value):
            i0, i1 = order(i0, i1)
            ref[index_of(m), (i0 * 5 + i1) * 10 + comp] = value

        return write

    line = [(0, j) for j in range(5)]

    def leaf_read(side, b0, b1, b2):
        base = pl.multiple_of((b1 * 8 + b2) * 32 + side * 8, 8)
        return leaf_ref[pl.ds(base, 8), :], leaf_ref[pl.ds(base + 16, 8), :]

    merge(
        0, [(0, 2), (1, 2)], 1, leaf_read,
        lambda m, side, b0, b1: [first_s[side * 20 + b1 * 4 + k] for k in range(4)],
        lambda i, side, j: float(CHILD[side][i, j]),
        writer(wa_ref, lambda m: 0), lambda v: v,
    )
    merge(
        1, line, 1, reader(wa_ref, 0), turner(lambda m: 0), chosen((sub >> 2 & 1) == 1),
        writer(wb_ref, lambda m: 0), lambda v: v + pltpu.roll(v, 4, 0),
    )
    merge(
        0, line, 1, reader(wb_ref, 0), turner(lambda m: 1), chosen((sub >> 1 & 1) == 1),
        writer(wa_ref, lambda m: 0), lambda v: v + pltpu.roll(v, 2, 0),
    )
    even = (sub & 1) == 0
    merge(
        1, line, 1, reader(wa_ref, 0), turner(lambda m: 2), chosen((sub & 1) == 1),
        writer(wb_ref, lambda m: 0),
        lambda v: v + jnp.where(even, pltpu.roll(v, 7, 0), pltpu.roll(v, 1, 0)),
    )
    order = flipped(0, a >> 2 & 1)
    merge(
        0, line, 1, reader(wb_ref, 0, order), turner(lambda m: 3, order), lower,
        writer(wa_ref, lambda m: 0, order), lambda v: v,
    )
    order = flipped(1, b >> 2 & 1)
    merge(
        1, line, 1, reader(wa_ref, 0, order), turner(lambda m: 4, order), lower,
        writer(wb_ref, lambda m: 0, order), lambda v: v,
    )
    order = flipped(0, a >> 3 & 1)
    merge(
        0, line, 2, reader(wb_ref, 0, order), turner(lambda m: 5 + m, order), lower,
        writer(wa_ref, lambda m: m, order), lambda v: v,
    )
    loads[0].wait()
    order = flipped(1, b >> 3 & 1)
    for k6 in range(2):
        merge(
            1, line, 2, reader(wa_ref, k6, order),
            turner((lambda k6: lambda m: 7 + 2 * k6 + m)(k6), order), lower,
            writer(wb_ref, (lambda k6: lambda m: 2 * k6 + m)(k6), order), lambda v: v,
        )

    loads[1].wait()
    loads[2].wait()
    scale = 1.0 / math.sqrt(GC * NF * N_INLINE * N_XLINE)
    for k67 in range(4):
        read = reader(wb_ref, k67)

        def body(b0, sums, k67=k67, read=read):
            sums = list(sums)
            for b1 in range(5):
                w = [read(0, b0, b1, b2) for b2 in range(5)]
                wp_re, wp_im = w[1][0] + w[3][0], w[1][1] + w[3][1]
                wm_re, wm_im = w[1][0] - w[3][0], w[1][1] - w[3][1]
                for m in range(2):
                    cu, su, cv, sv = (table_s[(11 + 2 * k67 + m) * 100 + (b0 * 5 + b1) * 4 + k] for k in range(4))
                    t_re, t_im = cmul(w[0][0], w[0][1], cu, su)
                    t_re = t_re + (w[2][0] + (cv * wp_re - sv * wm_im))
                    t_im = t_im + (w[2][1] + (cv * wp_im + sv * wm_re))
                    t_re, t_im = cmul(t_re, t_im, cu, su)
                    t_re, t_im = cmul(t_re + w[4][0], t_im + w[4][1], cu, su)
                    sums[2 * m] = sums[2 * m] + t_re
                    sums[2 * m + 1] = sums[2 * m + 1] + t_im
            return tuple(sums)

        sums = lax.fori_loop(0, 5, body, tuple(full(0.0) for _ in range(4)))
        for m in range(2):
            for part in range(2):
                out_ref[pl.ds(k67 * 32 + part * 2 + m, 8, stride=4), :] = sums[2 * m + part] * scale


def in_vmem():
    return pl.BlockSpec(memory_space=pltpu.VMEM)


def in_hbm():
    return pl.BlockSpec(memory_space=pltpu.HBM)


def device_place():
    return lax.axis_index("inline"), lax.axis_index("xline")


def told(body):
    def with_place(where_ref, *refs):
        body(lambda: (where_ref[0], where_ref[1]), *refs)

    return with_place


def run(body, where, in_specs, operands, **settings):
    if where is None:
        return pl.pallas_call(functools.partial(body, device_place), in_specs=in_specs, **settings)(*operands)
    return pl.pallas_call(
        told(body), in_specs=[pl.BlockSpec(memory_space=pltpu.SMEM)] + in_specs, interpret=True, **settings
    )(where, *operands)


def tables(where):
    return run(
        table_kernel,
        where,
        [],
        [],
        out_shape=[
            jax.ShapeDtypeStruct((NEAR * GC, 256, 128), BF16),
            jax.ShapeDtypeStruct((64, 8, 128), F32),
            pltpu.HBM(((16 - NEAR) * GC, 256, 128), BF16),
            pltpu.HBM((1200, 8, 128), F32),
        ],
        out_specs=[in_vmem(), in_vmem(), in_hbm(), in_hbm()],
        scratch_shapes=[
            pltpu.VMEM((15, 64, 128), F32),
            pltpu.VMEM(((16 - NEAR) * GC, 256, 128), BF16),
            pltpu.VMEM((1900, 8, 128), F32),
            pltpu.VMEM((1, 5, 8, 128), F32),
            pltpu.VMEM((1, 5, 8, 128), F32),
            pltpu.VMEM((1, 5, 8, 128), F32),
            pltpu.SemaphoreType.DMA((4,)),
        ],
        compiler_params=pltpu.CompilerParams(vmem_limit_bytes=14 << 20),
    )


def contributions(where, rows):
    near, turn, far, table = tables(where)
    if where is None:
        far = pltpu.with_memory_space_constraint(far, pltpu.HBM)
        table = pltpu.with_memory_space_constraint(table, pltpu.HBM)
    return run(
        kernel,
        where,
        [in_vmem(), in_vmem(), in_vmem(), in_hbm(), in_hbm()],
        [rows, near, turn, far, table],
        out_shape=jax.ShapeDtypeStruct((128, 128), F32),
        out_specs=in_vmem(),
        scratch_shapes=[
            pltpu.VMEM((2, 2, 16, 8, 128), F32),
            pltpu.VMEM((1280, 128), F32),
            pltpu.VMEM((2, 250, 8, 128), F32),
            pltpu.VMEM((4, 250, 8, 128), F32),
            pltpu.VMEM((100, 8, 128), F32),
            pltpu.VMEM(((16 - NEAR) * GC, 256, 128), BF16),
            pltpu.VMEM((1900, 8, 128), F32),
            pltpu.VMEM((40, 8, 128), F32),
            pltpu.VMEM((8, 5, 8, 128), F32),
            pltpu.VMEM((8, 5, 8, 128), F32),
            pltpu.VMEM((8, 5, 8, 128), F32),
            pltpu.SemaphoreType.DMA((4,)),
        ],
        compiler_params=pltpu.CompilerParams(vmem_limit_bytes=20 << 20),
    )


def shards(samples):
    rows = samples.reshape(1, 16, 128)
    rows = jnp.broadcast_to(rows, (16, 16, 128))
    rows = lax.all_to_all(rows, AXES, 0, 0, axis_index_groups=gather_groups())
    parts = contributions(None, rows).reshape(32, 4, 128)
    parts = lax.all_to_all(parts, AXES, 0, 0, axis_index_groups=scatter_groups())
    return jnp.sum(parts, axis=0).reshape(2, COLS)


def solution(mesh):
    return jax.shard_map(
        shards,
        mesh=mesh,
        in_specs=(P(None, "inline", "xline"),),
        out_specs=P(None, AXES),
        check_vma=False,
    )
```

```python
import functools
import math

import jax
import jax.numpy as jnp
import numpy as np
from jax import lax
from jax.experimental import pallas as pl
from jax.experimental.pallas import tpu as pltpu
from jax.sharding import PartitionSpec as P

NF = 256
COLS = 256
GC = 4
N_INLINE = 32
N_XLINE = 16
KAPPA = 40.0
AXES = ("inline", "xline")
F32 = jnp.float32
BF16 = jnp.bfloat16

ROOT = math.sqrt(0.5)
NODES = 0.5 * np.array([1.0, ROOT, 0.0, -ROOT, -1.0])


def basis_at(points):
    rows = []
    for k in range(5):
        factor = np.ones_like(points)
        for j in range(5):
            if j != k:
                factor = factor * (points - NODES[j]) / (NODES[k] - NODES[j])
        rows.append(factor)
    return np.stack(rows)


CHILD = [basis_at((t - 0.5) * 0.5 + 0.5 * NODES) for t in (0, 1)]
LEAF_XLINE = basis_at((np.arange(GC) + 0.5) / GC - 0.5)


def gather_groups():
    groups = []
    for base in range(N_INLINE * N_XLINE):
        a, b = base // N_XLINE, base % N_XLINE
        if a & 3 or b & 3:
            continue
        members = []
        for j in range(16):
            a0, b0, a1, b1 = j >> 3 & 1, j >> 2 & 1, j >> 1 & 1, j & 1
            members.append((a | a0 | a1 << 1) * N_XLINE + (b | b0 | b1 << 1))
        groups.append(members)
    return groups


def scatter_groups():
    groups = []
    for base in range(N_INLINE * N_XLINE):
        a, b = base // N_XLINE, base % N_XLINE
        if a >> 2 or b >> 2:
            continue
        members = []
        for j in range(32):
            k6, k7, k5, k3, k4 = j >> 4 & 1, j >> 3 & 1, j >> 2 & 1, j >> 1 & 1, j & 1
            members.append(
                (a | k3 << 2 | k5 << 3 | k7 << 4) * N_XLINE + (b | k4 << 2 | k6 << 3)
            )
        groups.append(members)
    return groups


def series(scale, bound, odd):
    coefs = []
    n = 0
    while True:
        power = 2 * n + (1 if odd else 0)
        size = (scale * bound) ** power / math.factorial(power)
        if size < 3e-8:
            return coefs
        coefs.append((-1.0) ** n * scale**power / math.factorial(power))
        n += 1


def poly(coefs, square):
    total = square * coefs[-1] + coefs[-2]
    for coef in coefs[-3::-1]:
        total = total * square + coef
    return total


def sincos_small(r, scale, bound):
    square = r * r
    return r * poly(series(scale, bound, True), square), poly(series(scale, bound, False), square)


def sincos_wide(x):
    turns = jnp.floor(x * (2.0 / math.pi) + 0.5)
    r = x - turns * 1.5703125
    r = r - turns * 4.837512969970703125e-4
    r = r - turns * 7.54978995489188216e-8
    sine, cosine = sincos_small(r, 1.0, 0.8)
    quarter = turns.astype(jnp.int32)
    swap = (quarter & 1) == 1
    s = jnp.where(swap, cosine, sine)
    c = jnp.where(swap, sine, cosine)
    s = jnp.where((quarter & 2) == 2, -s, s)
    c = jnp.where(((quarter + 1) & 2) == 2, -c, c)
    return s, c


def cmul(ar, ai, br, bi):
    return ar * br - ai * bi, ar * bi + ai * br


def full(value):
    return jnp.full((8, 128), value, F32)


def spot(bit):
    return (2 * bit - 1).astype(F32)


def places(where):
    a, b = where()
    lane = lax.broadcasted_iota(jnp.int32, (8, 128), 1)
    sub = lax.broadcasted_iota(jnp.int32, (8, 128), 0)
    column = lane + ((a & 1) << 7)

    def digits(where):
        coord = full(0.5 * 0.5 ** len(where))
        for rank, place in enumerate(where):
            coord = coord + (column >> place & 1).astype(F32) * 0.5 ** (rank + 1)
        return coord

    return a, b, lane, sub, (digits((7, 4, 1)), digits((6, 3, 0)), digits((5, 2)))


def five(factor):
    c1, s1, cv, sv = factor
    c2 = c1 * c1 - s1 * s1
    s2 = c1 * s1
    s2 = s2 + s2
    c3, s3 = cmul(c2, s2, c1, s1)
    cc, ss, cs, sc = c2 * cv, s2 * sv, c2 * sv, s2 * cv
    return [(c3, s3), (cc - ss, sc + cs), (c2, s2), (cc + ss, sc - cs), (c1, s1)]


NEAR = 11
STRETCHES = ((7, 11), (11, 15), (15, 19))


def stretch(k, table, held, sem, out):
    low, high = STRETCHES[k]
    far = table.at[pl.ds((low - 7) * 100, (high - low) * 100)]
    near = held.at[pl.ds(low * 100, (high - low) * 100)]
    return pltpu.make_async_copy(near, far, sem) if out else pltpu.make_async_copy(far, near, sem)


def plan(a, b, sub, centre):
    g0, g1, g2 = centre
    bit2, bit1, bit0, none = sub >> 2 & 1, sub >> 1 & 1, sub & 1, sub * 0
    a_base = a & ~3
    b_base = b & ~3
    unit_b = (b_base + bit2 + 2 * bit0).astype(F32) * (1.0 / N_XLINE)
    unit_a = (a_base + 2 * bit1).astype(F32) * (1.0 / N_INLINE)
    low_b = (b_base + 2 * bit0).astype(F32) * (1.0 / N_XLINE)

    def inline_low(bits):
        return (none + (a >> bits << bits)).astype(F32) * (1.0 / N_INLINE)

    def xline_low(bits):
        return (none + (b >> bits << bits)).astype(F32) * (1.0 / N_XLINE)

    levels = []
    sign = spot(none + (b & 1))
    for side in range(2):
        box = (unit_a + side / N_INLINE, 1.0 / N_INLINE, unit_b, 1.0 / N_XLINE)
        levels.append((box, (g0, g1, g2), 2, 2.0**-4, [sign], side))
    g2 = g2 + sign * 2.0**-4
    sign = spot(none + (a >> 1 & 1))
    box = (unit_a, 2.0 / N_INLINE, unit_b, 1.0 / N_XLINE)
    levels.append((box, (g0, g1, g2), 0, 2.0**-5, [sign], 0))
    g0 = g0 + sign * 2.0**-5
    sign = spot(none + (b >> 1 & 1))
    box = (unit_a, 2.0 / N_INLINE, low_b, 2.0 / N_XLINE)
    levels.append((box, (g0, g1, g2), 1, 2.0**-5, [sign], 1))
    g1 = g1 + sign * 2.0**-5
    sign = spot(bit1)
    box = (inline_low(2), 4.0 / N_INLINE, low_b, 2.0 / N_XLINE)
    levels.append((box, (g0, g1, g2), 2, 2.0**-5, [sign], 2))
    g2 = g2 + sign * 2.0**-5
    sign = spot(bit0)
    box = (inline_low(2), 4.0 / N_INLINE, xline_low(2), 4.0 / N_XLINE)
    levels.append((box, (g0, g1, g2), 0, 2.0**-6, [sign], 3))
    g0 = g0 + sign * 2.0**-6
    sign = spot(bit2)
    box = (inline_low(3), 8.0 / N_INLINE, xline_low(2), 4.0 / N_XLINE)
    levels.append((box, (g0, g1, g2), 1, 2.0**-6, [sign], 4))
    g1 = g1 + sign * 2.0**-6
    box = (inline_low(3), 8.0 / N_INLINE, xline_low(3), 8.0 / N_XLINE)
    levels.append((box, (g0, g1, g2), 2, 2.0**-6, [-1.0, 1.0], 5))
    for k6 in range(2):
        box = (inline_low(4), 16.0 / N_INLINE, xline_low(3), 8.0 / N_XLINE)
        centre = (g0, g1, g2 + (2 * k6 - 1) * 2.0**-6)
        levels.append((box, centre, 0, 2.0**-7, [-1.0, 1.0], 7 + 2 * k6))
    for k6 in range(2):
        for k7 in range(2):
            box = (inline_low(4), 16.0 / N_INLINE, full(0.0), 16.0 / N_XLINE)
            centre = (g0 + (2 * k7 - 1) * 2.0**-7, g1, g2 + (2 * k6 - 1) * 2.0**-6)
            levels.append((box, centre, 1, 2.0**-7, [-1.0, 1.0], 11 + 4 * k6 + 2 * k7))
    return levels


def turning(level, slot, p_ref, q_ref, s_ref, store, part=None):
    (low0, width0, low1, width1), centre, dim, q, signs, first = level
    anchor = 0.5 + centre[0]
    for k in range(5):
        place = float(NODES[k]) + 0.5
        x0 = (low0 + width0 * place) * (low0 + width0 * place)
        x1 = (low1 + width1 * place) * (low1 + width1 * place)
        p_ref[slot, k] = anchor * anchor + centre[1] * x0
        q_ref[slot, k] = centre[2] * x1
        if dim:
            s_ref[slot, k] = (x0 if dim == 1 else x1) * q
    for m, sign in enumerate(signs):
        if dim == 0:
            s_ref[slot, m] = 2.0 * q * sign * anchor + q * q

    def point(b0, b1):
        radicand = p_ref[slot, b0] + q_ref[slot, b1]
        root = radicand * lax.rsqrt(radicand)
        for m, sign in enumerate(signs):
            if dim == 0:
                moved = radicand + s_ref[slot, m]
            else:
                gap = s_ref[slot, b0 if dim == 1 else b1]
                if isinstance(sign, float):
                    moved = radicand + gap if sign > 0 else radicand - gap
                else:
                    moved = radicand + sign * gap
            change = moved * lax.rsqrt(moved) - root
            if part is not None:
                change = change * part
            s_u, c_u = sincos_small(change, 0.5 * KAPPA, q)
            s_v, c_v = sincos_small(change, KAPPA * float(NODES[1]), q)
            store(first + m, b0, b1, (c_u, s_u, c_v, s_v))

    return point


def table_kernel(where, near_ref, turn_ref, far_ref, table_ref, tab_ref, far_s, table_s, p_ref, q_ref, s_ref, sems):
    a, b, lane, sub, (g0, g1, g2) = places(where)
    bit2 = sub >> 2 & 1
    bit1 = sub >> 1 & 1
    bit0 = sub & 1
    a_base = a & ~3
    b_base = b & ~3

    for half in range(2):
        box_a = (a_base + half + 2 * bit1).astype(F32)
        box_b = (b_base + bit2 + 2 * bit0).astype(F32)
        x0 = (box_a + 0.5) * (1.0 / N_INLINE)
        part = (0.5 + g0) * (0.5 + g0) + g1 * (x0 * x0)
        for c in range(GC):
            at = pl.ds(c * 16 + half * 8, 8)
            x1 = (box_b + (c + 0.5) / GC) * (1.0 / N_XLINE)
            radicand = part + g2 * (x1 * x1)
            step = (KAPPA / NF) * (radicand * lax.rsqrt(radicand))
            tab_ref[0, at, :] = step
            s, co = sincos_wide(step * 132.0)
            s64, c64 = sincos_wide(step * 64.0)
            for f1 in range(4):
                turn_ref[f1 * 16 + c * 2 + half] = co
                turn_ref[f1 * 16 + 8 + c * 2 + half] = s
                if f1 < 3:
                    co, s = cmul(co, s, c64, s64)
            s8, c8 = sincos_wide(step * 8.0)
            co, s = c8, s8
            for f2 in range(1, 8):
                tab_ref[2 * f2 - 1, at, :] = co
                tab_ref[2 * f2, at, :] = s
                if f2 < 7:
                    co, s = cmul(co, s, c8, s8)

    offset = sub.astype(F32) - 3.5

    def wave(box, ref, first):
        for c in range(GC):
            row = c * 16 + box

            def table(i):
                return jnp.broadcast_to(tab_ref[i, pl.ds(row, 1), :], (8, 128))

            s_a, c_a = sincos_small(table(0) * offset, 1.0, 1.15)
            cos_rows, sin_rows = [c_a], [s_a]
            for f2 in range(1, 8):
                cr, sr = cmul(c_a, s_a, table(2 * f2 - 1), table(2 * f2))
                cos_rows.append(cr)
                sin_rows.append(sr)
            right = jnp.concatenate(cos_rows + sin_rows, axis=0)
            right_hi = right.astype(BF16)
            ref[(box - first) * GC + c, 0:128, :] = right_hi
            ref[(box - first) * GC + c, 128:256, :] = (right - right_hi.astype(F32)).astype(BF16)

    def far_wave(box, carry):
        wave(box, far_s, NEAR)
        return carry

    def near_wave(box, carry):
        wave(box, near_ref, 0)
        return carry

    lax.fori_loop(NEAR, 16, far_wave, 0, unroll=True)
    save_far = pltpu.make_async_copy(far_s, far_ref, sems.at[3])
    save_far.start()

    def held(index, b0, b1, factor):
        for k in range(4):
            table_s[index * 100 + (b0 * 5 + b1) * 4 + k] = factor[k]

    saves = []
    for i, level in enumerate(plan(a, b, sub, (g0, g1, g2))[8:]):
        point = turning(level, 0, p_ref, q_ref, s_ref, held)

        def across(b1, carry, point=point):
            for b0 in range(5):
                point(b0, b1)
            return carry

        lax.fori_loop(0, 5, across, 0, unroll=True)
        if i % 2:
            k = i // 2
            saves.append(stretch(k, table_ref, table_s, sems.at[k], True))
            saves[-1].start()
    lax.fori_loop(0, NEAR, near_wave, 0, unroll=True)
    save_far.wait()
    for copy in saves:
        copy.wait()


def kernel(where, rows_ref, near_ref, turn_ref, far_ref, table_ref, out_ref, v_ref, leaf_ref, wa_ref, wb_ref, x_ref, far_s, table_s, first_s, p_ref, q_ref, s_ref, sems):
    load_far = pltpu.make_async_copy(far_ref, far_s, sems.at[3])
    load_far.start()
    loads = [stretch(k, table_ref, table_s, sems.at[k], False) for k in range(3)]
    for load in loads:
        load.start()
    a, b, lane, sub, kept = places(where)

    def hold_first(side, b0, b1, factor):
        for k in range(4):
            first_s[side * 20 + b1 * 4 + k] = factor[k]

    def hold(index, b0, b1, factor):
        for k in range(4):
            table_s[index * 100 + (b0 * 5 + b1) * 4 + k] = factor[k]

    upper = (sub >> 2 & 1) == 1
    part = jnp.where(upper, 1.0, -1.0)

    points = []
    for i, level in enumerate(plan(a, b, sub, kept)[:8]):
        point = turning(
            level, i, p_ref, q_ref, s_ref, hold_first if i < 2 else hold, part if i in (3, 4, 5) else None
        )
        points += [(point, b0, b1) for b0 in ((2,) if i < 2 else range(5)) for b1 in range(5)]

    left = lax.broadcasted_iota(jnp.int32, (16, 8, 128), 2) < 64
    re = rows_ref[:, 0:8, :]
    im = rows_ref[:, 8:16, :]
    re_r = pltpu.roll(re, 64, 2)
    im_r = pltpu.roll(im, 64, 2)
    v_ref[0, 0] = jnp.where(left, re, -im_r)
    v_ref[1, 0] = jnp.where(left, re_r, -im)
    v_ref[0, 1] = jnp.where(left, im, re_r)
    v_ref[1, 1] = jnp.where(left, im_r, re)

    basis = []
    for f1 in range(4):
        z = ((lane & 63).astype(F32) + (f1 * 64 + 0.5)) * (1.0 / NF) - 0.5
        factor = jnp.zeros((8, 128), F32)
        for k in range(5):
            scale = 1.0
            for j in range(5):
                if j != k:
                    scale = scale / (NODES[k] - NODES[j])
            factor = jnp.where(sub == k, scale, factor)
        for j in range(5):
            factor = factor * jnp.where(sub == j, 1.0, z - NODES[j])
        basis.append(factor)

    def leaf_one(box):
        totals = []
        for c in range(GC):
            def table(i):
                return jnp.broadcast_to(turn_ref[i * 8 + c * 2 + box // 8, pl.ds(box % 8, 1), :], (8, 128))

            rows = []
            for f1 in range(4):
                for part in range(2):
                    sample = v_ref[f1 & 1, part, pl.ds(box, 1), 2 * c + f1 // 2, :]
                    rows.append(basis[f1] * jnp.broadcast_to(sample, (8, 128)))
            lhs = jnp.concatenate(rows, axis=0)
            lhs_hi = lhs.astype(BF16)
            lhs_lo = (lhs - lhs_hi.astype(F32)).astype(BF16)
            both = jnp.concatenate([lhs_hi, lhs_hi], axis=1)
            right = near_ref[box * GC + c] if box < NEAR else far_s[(box - NEAR) * GC + c]
            mixed = jnp.dot(both, right, preferred_element_type=F32)
            mixed = mixed + jnp.dot(lhs_lo, right[0:128], preferred_element_type=F32)
            t_re = None
            for f1 in range(4):
                u_re = mixed[f1 * 16 : f1 * 16 + 8]
                u_im = mixed[f1 * 16 + 8 : f1 * 16 + 16]
                r_re, r_im = cmul(u_re, u_im, table(2 * f1), table(2 * f1 + 1))
                t_re, t_im = (r_re, r_im) if t_re is None else (t_re + r_re, t_im + r_im)
            totals.append((t_re, t_im))
        for a1 in range(5):
            for part in range(2):
                total = totals[0][part] * float(LEAF_XLINE[a1, 0])
                for c in range(1, GC):
                    total = total + totals[c][part] * float(LEAF_XLINE[a1, c])
                leaf_ref[pl.ds((a1 * 16 + part) * 16 + box, 8, stride=32), :] = total

    for box in range(16):
        if box == NEAR:
            load_far.wait()
        leaf_one(box)
        for point, b0, b1 in points[box::16]:
            point(b0, b1)

    def merge(axis, points, sets, read, turn, weight, write):
        def body(other, carry):
            for n, (side, p) in enumerate(points):
                b0, b1 = (p, other) if axis == 0 else (other, p)
                turns = [five(turn(m, side, b0, b1)) for m in range(sets)]
                for b2 in range(5):
                    w_re, w_im = read(side, b0, b1, b2)
                    for m in range(sets):
                        x_re, x_im = cmul(w_re, w_im, *turns[m][b2])
                        x_ref[(m * 5 + n) * 10 + 2 * b2] = x_re
                        x_ref[(m * 5 + n) * 10 + 2 * b2 + 1] = x_im
            for m in range(sets):
                for b2 in range(5):
                    items = [
                        [x_ref[(m * 5 + n) * 10 + 2 * b2 + k] for n in range(len(points))] for k in range(2)
                    ]
                    for i in range(5):
                        totals = []
                        for k in range(2):
                            total = None
                            for (side, p), item in zip(points, items[k]):
                                coef = weight(i, side, p)
                                if coef is None:
                                    continue
                                term = item if isinstance(coef, float) and coef == 1.0 else item * coef
                                total = term if total is None else total + term
                            totals.append(total)
                        i0, i1 = (i, other) if axis == 0 else (other, i)
                        write(m, i0, i1, b2, totals)
            return carry

        lax.fori_loop(0, 5, body, 0)

    def merge_packed(axis, weight, read, turn, write, combine):
        def body(other, carry):
            for b in range(5):
                b0, b1 = (b, other) if axis == 0 else (other, b)
                for b2, (co, sine) in enumerate(five(turn(0, 0, b0, b1))):
                    both = read(b0, b1, b2)
                    x_ref[b * 5 + b2] = both * co + pltpu.roll(both, 4, 0) * sine
            for b2 in range(5):
                items = [x_ref[b * 5 + b2] for b in range(5)]
                for i in range(5):
                    total = None
                    for b in range(5):
                        coef = weight(i, 0, b)
                        if coef is None:
                            continue
                        term = items[b] if isinstance(coef, float) and coef == 1.0 else items[b] * coef
                        total = term if total is None else total + term
                    i0, i1 = (i, other) if axis == 0 else (other, i)
                    write(i0, i1, b2, combine(total))
            return carry

        lax.fori_loop(0, 5, body, 0)

    def packed_reader(ref, order=None):
        def read(b0, b1, b2):
            b0, b1 = (b0, b1) if order is None else order(b0, b1)
            return ref[0, (b0 * 5 + b1) * 10 + b2]

        return read

    def packed_writer(ref, order=None):
        def write(i0, i1, b2, value):
            i0, i1 = (i0, i1) if order is None else order(i0, i1)
            ref[0, (i0 * 5 + i1) * 10 + b2] = value

        return write

    def unpacked_reader(ref, order):
        def read(side, b0, b1, b2):
            b0, b1 = order(b0, b1)
            both = ref[0, (b0 * 5 + b1) * 10 + b2]
            turned = pltpu.roll(both, 4, 0)
            return jnp.where(upper, turned, both), jnp.where(upper, both, turned)

        return read

    def chosen(mask):
        table = [
            [
                None
                if CHILD[0][i, j] == 0.0 and CHILD[1][i, j] == 0.0
                else jnp.where(mask, float(CHILD[1][i, j]), float(CHILD[0][i, j]))
                for j in range(5)
            ]
            for i in range(5)
        ]
        return lambda i, side, j: table[i][j]

    def lower(i, side, j):
        return None if CHILD[0][i, j] == 0.0 else float(CHILD[0][i, j])

    def flipped(axis, bit):
        def order(i0, i1):
            if axis == 0:
                return i0 + bit * (4 - 2 * i0), i1
            return i0, i1 + bit * (4 - 2 * i1)

        return order

    def same(i0, i1):
        return i0, i1

    def reader(ref, index, order=same):
        def read(side, b0, b1, b2):
            b0, b1 = order(b0, b1)
            at = (b0 * 5 + b1) * 10 + b2 * 2
            return ref[index, at], ref[index, at + 1]

        return read

    def turner(index_of, order=same):
        def turn(m, side, b0, b1):
            b0, b1 = order(b0, b1)
            at = index_of(m) * 100 + (b0 * 5 + b1) * 4
            return [table_s[at + k] for k in range(4)]

        return turn

    def writer(ref, index_of, order=same):
        def write(m, i0, i1, b2, totals):
            i0, i1 = order(i0, i1)
            for k in range(2):
                ref[index_of(m), (i0 * 5 + i1) * 10 + 2 * b2 + k] = totals[k]

        return write

    line = [(0, j) for j in range(5)]

    def leaf_read(side, b0, b1, b2):
        base = pl.multiple_of((b1 * 8 + b2) * 32 + side * 8, 8)
        return leaf_ref[pl.ds(base, 8), :], leaf_ref[pl.ds(base + 16, 8), :]

    merge(
        0, [(0, 2), (1, 2)], 1, leaf_read,
        lambda m, side, b0, b1: [first_s[side * 20 + b1 * 4 + k] for k in range(4)],
        lambda i, side, j: float(CHILD[side][i, j]),
        writer(wa_ref, lambda m: 0),
    )
    def pack(m, i0, i1, b2, totals):
        re, im = totals
        both = jnp.where(upper, im, re) + pltpu.roll(jnp.where(upper, re, im), 4, 0)
        wb_ref[0, (i0 * 5 + i1) * 10 + b2] = both

    merge(1, line, 1, reader(wa_ref, 0), turner(lambda m: 0), chosen(upper), pack)
    odd = (sub >> 1 & 1) == 1
    merge_packed(
        0, chosen(odd), packed_reader(wb_ref), turner(lambda m: 1), packed_writer(wa_ref),
        lambda v: v + jnp.where(odd, pltpu.roll(v, 2, 0), pltpu.roll(v, 6, 0)),
    )
    even = (sub & 1) == 0
    merge_packed(
        1, chosen((sub & 1) == 1), packed_reader(wa_ref), turner(lambda m: 2), packed_writer(wb_ref),
        lambda v: v + jnp.where(even, pltpu.roll(v, 7, 0), pltpu.roll(v, 1, 0)),
    )
    order = flipped(0, a >> 2 & 1)
    merge_packed(
        0, lower, packed_reader(wb_ref, order), turner(lambda m: 3, order), packed_writer(wa_ref, order),
        lambda v: v,
    )
    order = flipped(1, b >> 2 & 1)
    merge(
        1, line, 1, unpacked_reader(wa_ref, order), turner(lambda m: 4, order), lower,
        writer(wb_ref, lambda m: 0, order),
    )
    order = flipped(0, a >> 3 & 1)
    merge(
        0, line, 2, reader(wb_ref, 0, order), turner(lambda m: 5 + m, order), lower,
        writer(wa_ref, lambda m: m, order),
    )
    loads[0].wait()
    order = flipped(1, b >> 3 & 1)
    for k6 in range(2):
        merge(
            1, line, 2, reader(wa_ref, k6, order),
            turner((lambda k6: lambda m: 7 + 2 * k6 + m)(k6), order), lower,
            writer(wb_ref, (lambda k6: lambda m: 2 * k6 + m)(k6), order),
        )

    loads[1].wait()
    loads[2].wait()
    scale = 1.0 / math.sqrt(GC * NF * N_INLINE * N_XLINE)
    for k67 in range(4):
        read = reader(wb_ref, k67)

        def body(b0, sums, k67=k67, read=read):
            sums = list(sums)
            for b1 in range(5):
                w = [read(0, b0, b1, b2) for b2 in range(5)]
                wp_re, wp_im = w[1][0] + w[3][0], w[1][1] + w[3][1]
                wm_re, wm_im = w[1][0] - w[3][0], w[1][1] - w[3][1]
                for m in range(2):
                    cu, su, cv, sv = (table_s[(11 + 2 * k67 + m) * 100 + (b0 * 5 + b1) * 4 + k] for k in range(4))
                    t_re, t_im = cmul(w[0][0], w[0][1], cu, su)
                    t_re = t_re + (w[2][0] + (cv * wp_re - sv * wm_im))
                    t_im = t_im + (w[2][1] + (cv * wp_im + sv * wm_re))
                    t_re, t_im = cmul(t_re, t_im, cu, su)
                    t_re, t_im = cmul(t_re + w[4][0], t_im + w[4][1], cu, su)
                    sums[2 * m] = sums[2 * m] + t_re
                    sums[2 * m + 1] = sums[2 * m + 1] + t_im
            return tuple(sums)

        sums = lax.fori_loop(0, 5, body, tuple(full(0.0) for _ in range(4)))
        for m in range(2):
            for part in range(2):
                out_ref[pl.ds(k67 * 32 + part * 2 + m, 8, stride=4), :] = sums[2 * m + part] * scale


def in_vmem():
    return pl.BlockSpec(memory_space=pltpu.VMEM)


def in_hbm():
    return pl.BlockSpec(memory_space=pltpu.HBM)


def device_place():
    return lax.axis_index("inline"), lax.axis_index("xline")


def told(body):
    def with_place(where_ref, *refs):
        body(lambda: (where_ref[0], where_ref[1]), *refs)

    return with_place


def run(body, where, in_specs, operands, **settings):
    if where is None:
        return pl.pallas_call(functools.partial(body, device_place), in_specs=in_specs, **settings)(*operands)
    return pl.pallas_call(
        told(body), in_specs=[pl.BlockSpec(memory_space=pltpu.SMEM)] + in_specs, interpret=True, **settings
    )(where, *operands)


def tables(where):
    return run(
        table_kernel,
        where,
        [],
        [],
        out_shape=[
            jax.ShapeDtypeStruct((NEAR * GC, 256, 128), BF16),
            jax.ShapeDtypeStruct((64, 8, 128), F32),
            pltpu.HBM(((16 - NEAR) * GC, 256, 128), BF16),
            pltpu.HBM((1200, 8, 128), F32),
        ],
        out_specs=[in_vmem(), in_vmem(), in_hbm(), in_hbm()],
        scratch_shapes=[
            pltpu.VMEM((15, 64, 128), F32),
            pltpu.VMEM(((16 - NEAR) * GC, 256, 128), BF16),
            pltpu.VMEM((1900, 8, 128), F32),
            pltpu.VMEM((1, 5, 8, 128), F32),
            pltpu.VMEM((1, 5, 8, 128), F32),
            pltpu.VMEM((1, 5, 8, 128), F32),
            pltpu.SemaphoreType.DMA((4,)),
        ],
        compiler_params=pltpu.CompilerParams(vmem_limit_bytes=14 << 20),
    )


def contributions(where, rows):
    near, turn, far, table = tables(where)
    if where is None:
        far = pltpu.with_memory_space_constraint(far, pltpu.HBM)
        table = pltpu.with_memory_space_constraint(table, pltpu.HBM)
    return run(
        kernel,
        where,
        [in_vmem(), in_vmem(), in_vmem(), in_hbm(), in_hbm()],
        [rows, near, turn, far, table],
        out_shape=jax.ShapeDtypeStruct((128, 128), F32),
        out_specs=in_vmem(),
        scratch_shapes=[
            pltpu.VMEM((2, 2, 16, 8, 128), F32),
            pltpu.VMEM((1280, 128), F32),
            pltpu.VMEM((2, 250, 8, 128), F32),
            pltpu.VMEM((4, 250, 8, 128), F32),
            pltpu.VMEM((100, 8, 128), F32),
            pltpu.VMEM(((16 - NEAR) * GC, 256, 128), BF16),
            pltpu.VMEM((1900, 8, 128), F32),
            pltpu.VMEM((40, 8, 128), F32),
            pltpu.VMEM((8, 5, 8, 128), F32),
            pltpu.VMEM((8, 5, 8, 128), F32),
            pltpu.VMEM((8, 5, 8, 128), F32),
            pltpu.SemaphoreType.DMA((4,)),
        ],
        compiler_params=pltpu.CompilerParams(vmem_limit_bytes=20 << 20),
    )


def shards(samples):
    rows = samples.reshape(1, 16, 128)
    rows = jnp.broadcast_to(rows, (16, 16, 128))
    rows = lax.all_to_all(rows, AXES, 0, 0, axis_index_groups=gather_groups())
    parts = contributions(None, rows).reshape(32, 4, 128)
    parts = lax.all_to_all(parts, AXES, 0, 0, axis_index_groups=scatter_groups())
    return jnp.sum(parts, axis=0).reshape(2, COLS)


def solution(mesh):
    return jax.shard_map(
        shards,
        mesh=mesh,
        in_specs=(P(None, "inline", "xline"),),
        out_specs=P(None, AXES),
        check_vma=False,
    )
```

```python
import functools
import math

import jax
import jax.numpy as jnp
import numpy as np
from jax import lax
from jax.experimental import pallas as pl
from jax.experimental.pallas import tpu as pltpu
from jax.sharding import PartitionSpec as P

NF = 256
COLS = 256
GC = 4
N_INLINE = 32
N_XLINE = 16
KAPPA = 40.0
AXES = ("inline", "xline")
F32 = jnp.float32
BF16 = jnp.bfloat16

ROOT = math.sqrt(0.5)
NODES = 0.5 * np.array([1.0, ROOT, 0.0, -ROOT, -1.0])


def basis_at(points):
    rows = []
    for k in range(5):
        factor = np.ones_like(points)
        for j in range(5):
            if j != k:
                factor = factor * (points - NODES[j]) / (NODES[k] - NODES[j])
        rows.append(factor)
    return np.stack(rows)


CHILD = [basis_at((t - 0.5) * 0.5 + 0.5 * NODES) for t in (0, 1)]
LEAF_XLINE = basis_at((np.arange(GC) + 0.5) / GC - 0.5)


FIRST_LEAD = 15
LEAD = 25


def wanted(index, place):
    return (index ^ LEAD) >> place & 1


def gather_groups():
    groups = []
    for base in range(N_INLINE * N_XLINE):
        a, b = base // N_XLINE, base % N_XLINE
        if a & 3 or b & 3:
            continue
        members = []
        for j in range(16):
            a0, b0, a1, b1 = (((j ^ FIRST_LEAD) >> place) & 1 for place in (3, 2, 1, 0))
            members.append((a | a0 | a1 << 1) * N_XLINE + (b | b0 | b1 << 1))
        groups.append(members)
    return groups


def scatter_groups():
    groups = []
    for base in range(N_INLINE * N_XLINE):
        a, b = base // N_XLINE, base % N_XLINE
        if a >> 2 or b >> 2:
            continue
        members = []
        for j in range(32):
            k6, k7, k5, k3, k4 = (wanted(j, place) for place in (4, 3, 2, 1, 0))
            members.append(
                (a | k3 << 2 | k5 << 3 | k7 << 4) * N_XLINE + (b | k4 << 2 | k6 << 3)
            )
        groups.append(members)
    return groups


def series(scale, bound, odd):
    coefs = []
    n = 0
    while True:
        power = 2 * n + (1 if odd else 0)
        size = (scale * bound) ** power / math.factorial(power)
        if size < 3e-8:
            return coefs
        coefs.append((-1.0) ** n * scale**power / math.factorial(power))
        n += 1


def poly(coefs, square):
    total = square * coefs[-1] + coefs[-2]
    for coef in coefs[-3::-1]:
        total = total * square + coef
    return total


def sincos_small(r, scale, bound):
    square = r * r
    return r * poly(series(scale, bound, True), square), poly(series(scale, bound, False), square)


def sincos_wide(x):
    turns = jnp.floor(x * (2.0 / math.pi) + 0.5)
    r = x - turns * 1.5703125
    r = r - turns * 4.837512969970703125e-4
    r = r - turns * 7.54978995489188216e-8
    sine, cosine = sincos_small(r, 1.0, 0.8)
    quarter = turns.astype(jnp.int32)
    swap = (quarter & 1) == 1
    s = jnp.where(swap, cosine, sine)
    c = jnp.where(swap, sine, cosine)
    s = jnp.where((quarter & 2) == 2, -s, s)
    c = jnp.where(((quarter + 1) & 2) == 2, -c, c)
    return s, c


def cmul(ar, ai, br, bi):
    return ar * br - ai * bi, ar * bi + ai * br


def full(value):
    return jnp.full((8, 128), value, F32)


def spot(bit):
    return (2 * bit - 1).astype(F32)


def places(where):
    a, b = where()
    lane = lax.broadcasted_iota(jnp.int32, (8, 128), 1)
    sub = lax.broadcasted_iota(jnp.int32, (8, 128), 0)
    column = lane + ((a & 1) << 7)

    def digits(where):
        coord = full(0.5 * 0.5 ** len(where))
        for rank, place in enumerate(where):
            coord = coord + (column >> place & 1).astype(F32) * 0.5 ** (rank + 1)
        return coord

    return a, b, lane, sub, (digits((7, 4, 1)), digits((6, 3, 0)), digits((5, 2)))


def five(factor):
    c1, s1, cv, sv = factor
    c2 = c1 * c1 - s1 * s1
    s2 = c1 * s1
    s2 = s2 + s2
    c3, s3 = cmul(c2, s2, c1, s1)
    cc, ss, cs, sc = c2 * cv, s2 * sv, c2 * sv, s2 * cv
    return [(c3, s3), (cc - ss, sc + cs), (c2, s2), (cc + ss, sc - cs), (c1, s1)]


NEAR = 11
STRETCHES = ((7, 11), (11, 15), (15, 19))


def stretch(k, table, held, sem, out):
    low, high = STRETCHES[k]
    far = table.at[pl.ds((low - 7) * 100, (high - low) * 100)]
    near = held.at[pl.ds(low * 100, (high - low) * 100)]
    return pltpu.make_async_copy(near, far, sem) if out else pltpu.make_async_copy(far, near, sem)


def plan(a, b, sub, centre):
    g0, g1, g2 = centre
    bit2, bit1, bit0, none = sub >> 2 & 1, sub >> 1 & 1, sub & 1, sub * 0
    a_base = a & ~3
    b_base = b & ~3
    unit_b = (b_base + bit2 + 2 * bit0).astype(F32) * (1.0 / N_XLINE)
    unit_a = (a_base + 2 * bit1).astype(F32) * (1.0 / N_INLINE)
    low_b = (b_base + 2 * bit0).astype(F32) * (1.0 / N_XLINE)

    def inline_low(bits):
        return (none + (a >> bits << bits)).astype(F32) * (1.0 / N_INLINE)

    def xline_low(bits):
        return (none + (b >> bits << bits)).astype(F32) * (1.0 / N_XLINE)

    levels = []
    sign = spot(none + (b & 1))
    for side in range(2):
        box = (unit_a + side / N_INLINE, 1.0 / N_INLINE, unit_b, 1.0 / N_XLINE)
        levels.append((box, (g0, g1, g2), 2, 2.0**-4, [sign], side))
    g2 = g2 + sign * 2.0**-4
    sign = spot(none + (a >> 1 & 1))
    box = (unit_a, 2.0 / N_INLINE, unit_b, 1.0 / N_XLINE)
    levels.append((box, (g0, g1, g2), 0, 2.0**-5, [sign], 0))
    g0 = g0 + sign * 2.0**-5
    sign = spot(none + (b >> 1 & 1))
    box = (unit_a, 2.0 / N_INLINE, low_b, 2.0 / N_XLINE)
    levels.append((box, (g0, g1, g2), 1, 2.0**-5, [sign], 1))
    g1 = g1 + sign * 2.0**-5
    sign = spot(bit1 ^ wanted(0, 1))
    box = (inline_low(2), 4.0 / N_INLINE, low_b, 2.0 / N_XLINE)
    levels.append((box, (g0, g1, g2), 2, 2.0**-5, [sign], 2))
    g2 = g2 + sign * 2.0**-5
    sign = spot(bit0 ^ wanted(0, 0))
    box = (inline_low(2), 4.0 / N_INLINE, xline_low(2), 4.0 / N_XLINE)
    levels.append((box, (g0, g1, g2), 0, 2.0**-6, [sign], 3))
    g0 = g0 + sign * 2.0**-6
    sign = spot(bit2 ^ wanted(0, 2))
    box = (inline_low(3), 8.0 / N_INLINE, xline_low(2), 4.0 / N_XLINE)
    levels.append((box, (g0, g1, g2), 1, 2.0**-6, [sign], 4))
    g1 = g1 + sign * 2.0**-6
    box = (inline_low(3), 8.0 / N_INLINE, xline_low(3), 8.0 / N_XLINE)
    signs = [2.0 * wanted(k << 4, 4) - 1.0 for k in range(2)]
    levels.append((box, (g0, g1, g2), 2, 2.0**-6, signs, 5))
    next_signs = [2.0 * wanted(k << 3, 3) - 1.0 for k in range(2)]
    for k6 in range(2):
        box = (inline_low(4), 16.0 / N_INLINE, xline_low(3), 8.0 / N_XLINE)
        centre = (g0, g1, g2 + signs[k6] * 2.0**-6)
        levels.append((box, centre, 0, 2.0**-7, next_signs, 7 + 2 * k6))
    for k6 in range(2):
        for k7 in range(2):
            box = (inline_low(4), 16.0 / N_INLINE, full(0.0), 16.0 / N_XLINE)
            centre = (g0 + next_signs[k7] * 2.0**-7, g1, g2 + signs[k6] * 2.0**-6)
            levels.append((box, centre, 1, 2.0**-7, [-1.0, 1.0], 11 + 4 * k6 + 2 * k7))
    return levels


def turning(level, slot, p_ref, q_ref, s_ref, store, part=None):
    (low0, width0, low1, width1), centre, dim, q, signs, first = level
    anchor = 0.5 + centre[0]
    for k in range(5):
        place = float(NODES[k]) + 0.5
        x0 = (low0 + width0 * place) * (low0 + width0 * place)
        x1 = (low1 + width1 * place) * (low1 + width1 * place)
        p_ref[slot, k] = anchor * anchor + centre[1] * x0
        q_ref[slot, k] = centre[2] * x1
        if dim:
            s_ref[slot, k] = (x0 if dim == 1 else x1) * q
    for m, sign in enumerate(signs):
        if dim == 0:
            s_ref[slot, m] = 2.0 * q * sign * anchor + q * q

    def point(b0, b1):
        radicand = p_ref[slot, b0] + q_ref[slot, b1]
        root = radicand * lax.rsqrt(radicand)
        for m, sign in enumerate(signs):
            if dim == 0:
                moved = radicand + s_ref[slot, m]
            else:
                gap = s_ref[slot, b0 if dim == 1 else b1]
                if isinstance(sign, float):
                    moved = radicand + gap if sign > 0 else radicand - gap
                else:
                    moved = radicand + sign * gap
            change = moved * lax.rsqrt(moved) - root
            if part is not None:
                change = change * part
            s_u, c_u = sincos_small(change, 0.5 * KAPPA, q)
            s_v, c_v = sincos_small(change, KAPPA * float(NODES[1]), q)
            store(first + m, b0, b1, (c_u, s_u, c_v, s_v))

    return point


def table_kernel(where, near_ref, turn_ref, far_ref, table_ref, tab_ref, far_s, table_s, p_ref, q_ref, s_ref, sems):
    a, b, lane, sub, (g0, g1, g2) = places(where)
    bit2 = sub >> 2 & 1
    bit1 = sub >> 1 & 1
    bit0 = sub & 1
    a_base = a & ~3
    b_base = b & ~3

    for half in range(2):
        box_a = (a_base + half + 2 * bit1).astype(F32)
        box_b = (b_base + bit2 + 2 * bit0).astype(F32)
        x0 = (box_a + 0.5) * (1.0 / N_INLINE)
        part = (0.5 + g0) * (0.5 + g0) + g1 * (x0 * x0)
        for c in range(GC):
            at = pl.ds(c * 16 + half * 8, 8)
            x1 = (box_b + (c + 0.5) / GC) * (1.0 / N_XLINE)
            radicand = part + g2 * (x1 * x1)
            step = (KAPPA / NF) * (radicand * lax.rsqrt(radicand))
            tab_ref[0, at, :] = step
            s, co = sincos_wide(step * 132.0)
            s64, c64 = sincos_wide(step * 64.0)
            for f1 in range(4):
                turn_ref[f1 * 16 + c * 2 + half] = co
                turn_ref[f1 * 16 + 8 + c * 2 + half] = s
                if f1 < 3:
                    co, s = cmul(co, s, c64, s64)
            s8, c8 = sincos_wide(step * 8.0)
            co, s = c8, s8
            for f2 in range(1, 8):
                tab_ref[2 * f2 - 1, at, :] = co
                tab_ref[2 * f2, at, :] = s
                if f2 < 7:
                    co, s = cmul(co, s, c8, s8)

    offset = sub.astype(F32) - 3.5

    def wave(box, ref, first):
        for c in range(GC):
            row = c * 16 + box

            def table(i):
                return jnp.broadcast_to(tab_ref[i, pl.ds(row, 1), :], (8, 128))

            s_a, c_a = sincos_small(table(0) * offset, 1.0, 1.15)
            cos_rows, sin_rows = [c_a], [s_a]
            for f2 in range(1, 8):
                cr, sr = cmul(c_a, s_a, table(2 * f2 - 1), table(2 * f2))
                cos_rows.append(cr)
                sin_rows.append(sr)
            right = jnp.concatenate(cos_rows + sin_rows, axis=0)
            right_hi = right.astype(BF16)
            ref[(box - first) * GC + c, 0:128, :] = right_hi
            ref[(box - first) * GC + c, 128:256, :] = (right - right_hi.astype(F32)).astype(BF16)

    def far_wave(box, carry):
        wave(box, far_s, NEAR)
        return carry

    def near_wave(box, carry):
        wave(box, near_ref, 0)
        return carry

    lax.fori_loop(NEAR, 16, far_wave, 0, unroll=True)
    save_far = pltpu.make_async_copy(far_s, far_ref, sems.at[3])
    save_far.start()

    def held(index, b0, b1, factor):
        for k in range(4):
            table_s[index * 100 + (b0 * 5 + b1) * 4 + k] = factor[k]

    saves = []
    for i, level in enumerate(plan(a, b, sub, (g0, g1, g2))[8:]):
        point = turning(level, 0, p_ref, q_ref, s_ref, held)

        def across(b1, carry, point=point):
            for b0 in range(5):
                point(b0, b1)
            return carry

        lax.fori_loop(0, 5, across, 0, unroll=True)
        if i % 2:
            k = i // 2
            saves.append(stretch(k, table_ref, table_s, sems.at[k], True))
            saves[-1].start()
    lax.fori_loop(0, NEAR, near_wave, 0, unroll=True)
    save_far.wait()
    for copy in saves:
        copy.wait()


def kernel(where, rows_ref, near_ref, turn_ref, far_ref, table_ref, out_ref, v_ref, leaf_ref, wa_ref, wb_ref, x_ref, far_s, table_s, first_s, p_ref, q_ref, s_ref, sems):
    load_far = pltpu.make_async_copy(far_ref, far_s, sems.at[3])
    load_far.start()
    loads = [stretch(k, table_ref, table_s, sems.at[k], False) for k in range(3)]
    for load in loads:
        load.start()
    a, b, lane, sub, kept = places(where)

    def hold_first(side, b0, b1, factor):
        for k in range(4):
            first_s[side * 20 + b1 * 4 + k] = factor[k]

    def hold(index, b0, b1, factor):
        for k in range(4):
            table_s[index * 100 + (b0 * 5 + b1) * 4 + k] = factor[k]

    upper = (sub >> 2 & 1) == 1
    part = jnp.where(upper, 1.0, -1.0)

    points = []
    for i, level in enumerate(plan(a, b, sub, kept)[:8]):
        point = turning(
            level, i, p_ref, q_ref, s_ref, hold_first if i < 2 else hold, part if i in (3, 4, 5) else None
        )
        points += [(point, b0, b1) for b0 in ((2,) if i < 2 else range(5)) for b1 in range(5)]

    left = lax.broadcasted_iota(jnp.int32, (16, 8, 128), 2) < 64
    re = rows_ref[:, 0:8, :]
    im = rows_ref[:, 8:16, :]
    re_r = pltpu.roll(re, 64, 2)
    im_r = pltpu.roll(im, 64, 2)
    v_ref[0, 0] = jnp.where(left, re, -im_r)
    v_ref[1, 0] = jnp.where(left, re_r, -im)
    v_ref[0, 1] = jnp.where(left, im, re_r)
    v_ref[1, 1] = jnp.where(left, im_r, re)

    basis = []
    for f1 in range(4):
        z = ((lane & 63).astype(F32) + (f1 * 64 + 0.5)) * (1.0 / NF) - 0.5
        factor = jnp.zeros((8, 128), F32)
        for k in range(5):
            scale = 1.0
            for j in range(5):
                if j != k:
                    scale = scale / (NODES[k] - NODES[j])
            factor = jnp.where(sub == k, scale, factor)
        for j in range(5):
            factor = factor * jnp.where(sub == j, 1.0, z - NODES[j])
        basis.append(factor)

    def leaf_one(box):
        totals = []
        for c in range(GC):
            def table(i):
                return jnp.broadcast_to(turn_ref[i * 8 + c * 2 + box // 8, pl.ds(box % 8, 1), :], (8, 128))

            rows = []
            for f1 in range(4):
                for part in range(2):
                    sample = v_ref[f1 & 1, part, pl.ds(box ^ FIRST_LEAD, 1), 2 * c + f1 // 2, :]
                    rows.append(basis[f1] * jnp.broadcast_to(sample, (8, 128)))
            lhs = jnp.concatenate(rows, axis=0)
            lhs_hi = lhs.astype(BF16)
            lhs_lo = (lhs - lhs_hi.astype(F32)).astype(BF16)
            both = jnp.concatenate([lhs_hi, lhs_hi], axis=1)
            right = near_ref[box * GC + c] if box < NEAR else far_s[(box - NEAR) * GC + c]
            mixed = jnp.dot(both, right, preferred_element_type=F32)
            mixed = mixed + jnp.dot(lhs_lo, right[0:128], preferred_element_type=F32)
            t_re = None
            for f1 in range(4):
                u_re = mixed[f1 * 16 : f1 * 16 + 8]
                u_im = mixed[f1 * 16 + 8 : f1 * 16 + 16]
                r_re, r_im = cmul(u_re, u_im, table(2 * f1), table(2 * f1 + 1))
                t_re, t_im = (r_re, r_im) if t_re is None else (t_re + r_re, t_im + r_im)
            totals.append((t_re, t_im))
        for a1 in range(5):
            for part in range(2):
                total = totals[0][part] * float(LEAF_XLINE[a1, 0])
                for c in range(1, GC):
                    total = total + totals[c][part] * float(LEAF_XLINE[a1, c])
                leaf_ref[pl.ds((a1 * 16 + part) * 16 + box, 8, stride=32), :] = total

    for box in range(16):
        if box == NEAR:
            load_far.wait()
        leaf_one(box)
        for point, b0, b1 in points[box::16]:
            point(b0, b1)

    def merge(axis, points, sets, read, turn, weight, write):
        def body(other, carry):
            for n, (side, p) in enumerate(points):
                b0, b1 = (p, other) if axis == 0 else (other, p)
                turns = [five(turn(m, side, b0, b1)) for m in range(sets)]
                for b2 in range(5):
                    w_re, w_im = read(side, b0, b1, b2)
                    for m in range(sets):
                        x_re, x_im = cmul(w_re, w_im, *turns[m][b2])
                        x_ref[(m * 5 + n) * 10 + 2 * b2] = x_re
                        x_ref[(m * 5 + n) * 10 + 2 * b2 + 1] = x_im
            for m in range(sets):
                for b2 in range(5):
                    items = [
                        [x_ref[(m * 5 + n) * 10 + 2 * b2 + k] for n in range(len(points))] for k in range(2)
                    ]
                    for i in range(5):
                        totals = []
                        for k in range(2):
                            total = None
                            for (side, p), item in zip(points, items[k]):
                                coef = weight(i, side, p)
                                if coef is None:
                                    continue
                                term = item if isinstance(coef, float) and coef == 1.0 else item * coef
                                total = term if total is None else total + term
                            totals.append(total)
                        i0, i1 = (i, other) if axis == 0 else (other, i)
                        write(m, i0, i1, b2, totals)
            return carry

        lax.fori_loop(0, 5, body, 0)

    def merge_packed(axis, weight, read, turn, write, combine):
        def body(other, carry):
            for b in range(5):
                b0, b1 = (b, other) if axis == 0 else (other, b)
                for b2, (co, sine) in enumerate(five(turn(0, 0, b0, b1))):
                    both = read(b0, b1, b2)
                    x_ref[b * 5 + b2] = both * co + pltpu.roll(both, 4, 0) * sine
            for b2 in range(5):
                items = [x_ref[b * 5 + b2] for b in range(5)]
                for i in range(5):
                    total = None
                    for b in range(5):
                        coef = weight(i, 0, b)
                        if coef is None:
                            continue
                        term = items[b] if isinstance(coef, float) and coef == 1.0 else items[b] * coef
                        total = term if total is None else total + term
                    i0, i1 = (i, other) if axis == 0 else (other, i)
                    write(i0, i1, b2, combine(total))
            return carry

        lax.fori_loop(0, 5, body, 0)

    def packed_reader(ref, order=None):
        def read(b0, b1, b2):
            b0, b1 = (b0, b1) if order is None else order(b0, b1)
            return ref[0, (b0 * 5 + b1) * 10 + b2]

        return read

    def packed_writer(ref, order=None):
        def write(i0, i1, b2, value):
            i0, i1 = (i0, i1) if order is None else order(i0, i1)
            ref[0, (i0 * 5 + i1) * 10 + b2] = value

        return write

    def unpacked_reader(ref, order):
        def read(side, b0, b1, b2):
            b0, b1 = order(b0, b1)
            both = ref[0, (b0 * 5 + b1) * 10 + b2]
            turned = pltpu.roll(both, 4, 0)
            return jnp.where(upper, turned, both), jnp.where(upper, both, turned)

        return read

    def chosen(mask):
        table = [
            [
                None
                if CHILD[0][i, j] == 0.0 and CHILD[1][i, j] == 0.0
                else jnp.where(mask, float(CHILD[1][i, j]), float(CHILD[0][i, j]))
                for j in range(5)
            ]
            for i in range(5)
        ]
        return lambda i, side, j: table[i][j]

    def lower(i, side, j):
        return None if CHILD[0][i, j] == 0.0 else float(CHILD[0][i, j])

    def flipped(axis, bit):
        def order(i0, i1):
            if axis == 0:
                return i0 + bit * (4 - 2 * i0), i1
            return i0, i1 + bit * (4 - 2 * i1)

        return order

    def same(i0, i1):
        return i0, i1

    def reader(ref, index, order=same):
        def read(side, b0, b1, b2):
            b0, b1 = order(b0, b1)
            at = (b0 * 5 + b1) * 10 + b2 * 2
            return ref[index, at], ref[index, at + 1]

        return read

    def turner(index_of, order=same):
        def turn(m, side, b0, b1):
            b0, b1 = order(b0, b1)
            at = index_of(m) * 100 + (b0 * 5 + b1) * 4
            return [table_s[at + k] for k in range(4)]

        return turn

    def writer(ref, index_of, order=same):
        def write(m, i0, i1, b2, totals):
            i0, i1 = order(i0, i1)
            for k in range(2):
                ref[index_of(m), (i0 * 5 + i1) * 10 + 2 * b2 + k] = totals[k]

        return write

    line = [(0, j) for j in range(5)]

    def leaf_read(side, b0, b1, b2):
        base = pl.multiple_of((b1 * 8 + b2) * 32 + side * 8, 8)
        return leaf_ref[pl.ds(base, 8), :], leaf_ref[pl.ds(base + 16, 8), :]

    merge(
        0, [(0, 2), (1, 2)], 1, leaf_read,
        lambda m, side, b0, b1: [first_s[side * 20 + b1 * 4 + k] for k in range(4)],
        lambda i, side, j: float(CHILD[side][i, j]),
        writer(wa_ref, lambda m: 0),
    )
    def pack(m, i0, i1, b2, totals):
        re, im = totals
        both = jnp.where(upper, im, re) + pltpu.roll(jnp.where(upper, re, im), 4, 0)
        wb_ref[0, (i0 * 5 + i1) * 10 + b2] = both

    merge(1, line, 1, reader(wa_ref, 0), turner(lambda m: 0), chosen(upper), pack)
    odd = (sub >> 1 & 1) == 1
    merge_packed(
        0, chosen(odd), packed_reader(wb_ref), turner(lambda m: 1), packed_writer(wa_ref),
        lambda v: v + jnp.where(odd, pltpu.roll(v, 2, 0), pltpu.roll(v, 6, 0)),
    )
    even = (sub & 1) == 0
    merge_packed(
        1, chosen((sub & 1) == 1), packed_reader(wa_ref), turner(lambda m: 2), packed_writer(wb_ref),
        lambda v: v + jnp.where(even, pltpu.roll(v, 7, 0), pltpu.roll(v, 1, 0)),
    )
    order = flipped(0, a >> 2 & 1)
    merge_packed(
        0, lower, packed_reader(wb_ref, order), turner(lambda m: 3, order), packed_writer(wa_ref, order),
        lambda v: v,
    )
    order = flipped(1, b >> 2 & 1)
    merge(
        1, line, 1, unpacked_reader(wa_ref, order), turner(lambda m: 4, order), lower,
        writer(wb_ref, lambda m: 0, order),
    )
    order = flipped(0, a >> 3 & 1)
    merge(
        0, line, 2, reader(wb_ref, 0, order), turner(lambda m: 5 + m, order), lower,
        writer(wa_ref, lambda m: m, order),
    )
    loads[0].wait()
    order = flipped(1, b >> 3 & 1)
    for k6 in range(2):
        merge(
            1, line, 2, reader(wa_ref, k6, order),
            turner((lambda k6: lambda m: 7 + 2 * k6 + m)(k6), order), lower,
            writer(wb_ref, (lambda k6: lambda m: 2 * k6 + m)(k6), order),
        )

    loads[1].wait()
    loads[2].wait()
    scale = 1.0 / math.sqrt(GC * NF * N_INLINE * N_XLINE)
    for k67 in range(4):
        read = reader(wb_ref, k67)

        def body(b0, sums, k67=k67, read=read):
            sums = list(sums)
            for b1 in range(5):
                w = [read(0, b0, b1, b2) for b2 in range(5)]
                wp_re, wp_im = w[1][0] + w[3][0], w[1][1] + w[3][1]
                wm_re, wm_im = w[1][0] - w[3][0], w[1][1] - w[3][1]
                for m in range(2):
                    cu, su, cv, sv = (table_s[(11 + 2 * k67 + m) * 100 + (b0 * 5 + b1) * 4 + k] for k in range(4))
                    t_re, t_im = cmul(w[0][0], w[0][1], cu, su)
                    t_re = t_re + (w[2][0] + (cv * wp_re - sv * wm_im))
                    t_im = t_im + (w[2][1] + (cv * wp_im + sv * wm_re))
                    t_re, t_im = cmul(t_re, t_im, cu, su)
                    t_re, t_im = cmul(t_re + w[4][0], t_im + w[4][1], cu, su)
                    sums[2 * m] = sums[2 * m] + t_re
                    sums[2 * m + 1] = sums[2 * m + 1] + t_im
            return tuple(sums)

        sums = lax.fori_loop(0, 5, body, tuple(full(0.0) for _ in range(4)))
        for m in range(2):
            for part in range(2):
                out_ref[pl.ds(k67 * 32 + part * 2 + m, 8, stride=4), :] = sums[2 * m + part] * scale


def in_vmem():
    return pl.BlockSpec(memory_space=pltpu.VMEM)


def in_hbm():
    return pl.BlockSpec(memory_space=pltpu.HBM)


def device_place():
    return lax.axis_index("inline"), lax.axis_index("xline")


def told(body):
    def with_place(where_ref, *refs):
        body(lambda: (where_ref[0], where_ref[1]), *refs)

    return with_place


def run(body, where, in_specs, operands, **settings):
    if where is None:
        return pl.pallas_call(functools.partial(body, device_place), in_specs=in_specs, **settings)(*operands)
    return pl.pallas_call(
        told(body), in_specs=[pl.BlockSpec(memory_space=pltpu.SMEM)] + in_specs, interpret=True, **settings
    )(where, *operands)


def tables(where):
    return run(
        table_kernel,
        where,
        [],
        [],
        out_shape=[
            jax.ShapeDtypeStruct((NEAR * GC, 256, 128), BF16),
            jax.ShapeDtypeStruct((64, 8, 128), F32),
            pltpu.HBM(((16 - NEAR) * GC, 256, 128), BF16),
            pltpu.HBM((1200, 8, 128), F32),
        ],
        out_specs=[in_vmem(), in_vmem(), in_hbm(), in_hbm()],
        scratch_shapes=[
            pltpu.VMEM((15, 64, 128), F32),
            pltpu.VMEM(((16 - NEAR) * GC, 256, 128), BF16),
            pltpu.VMEM((1900, 8, 128), F32),
            pltpu.VMEM((1, 5, 8, 128), F32),
            pltpu.VMEM((1, 5, 8, 128), F32),
            pltpu.VMEM((1, 5, 8, 128), F32),
            pltpu.SemaphoreType.DMA((4,)),
        ],
        compiler_params=pltpu.CompilerParams(vmem_limit_bytes=14 << 20),
    )


def contributions(where, rows):
    near, turn, far, table = tables(where)
    if where is None:
        far = pltpu.with_memory_space_constraint(far, pltpu.HBM)
        table = pltpu.with_memory_space_constraint(table, pltpu.HBM)
    return run(
        kernel,
        where,
        [in_vmem(), in_vmem(), in_vmem(), in_hbm(), in_hbm()],
        [rows, near, turn, far, table],
        out_shape=jax.ShapeDtypeStruct((128, 128), F32),
        out_specs=in_vmem(),
        scratch_shapes=[
            pltpu.VMEM((2, 2, 16, 8, 128), F32),
            pltpu.VMEM((1280, 128), F32),
            pltpu.VMEM((2, 250, 8, 128), F32),
            pltpu.VMEM((4, 250, 8, 128), F32),
            pltpu.VMEM((100, 8, 128), F32),
            pltpu.VMEM(((16 - NEAR) * GC, 256, 128), BF16),
            pltpu.VMEM((1900, 8, 128), F32),
            pltpu.VMEM((40, 8, 128), F32),
            pltpu.VMEM((8, 5, 8, 128), F32),
            pltpu.VMEM((8, 5, 8, 128), F32),
            pltpu.VMEM((8, 5, 8, 128), F32),
            pltpu.SemaphoreType.DMA((4,)),
        ],
        compiler_params=pltpu.CompilerParams(vmem_limit_bytes=20 << 20),
    )


def shards(samples):
    rows = samples.reshape(1, 16, 128)
    rows = jnp.broadcast_to(rows, (16, 16, 128))
    rows = lax.all_to_all(rows, AXES, 0, 0, axis_index_groups=gather_groups())
    parts = contributions(None, rows).reshape(32, 4, 128)
    parts = lax.all_to_all(parts, AXES, 0, 0, axis_index_groups=scatter_groups())
    return jnp.sum(parts, axis=0).reshape(2, COLS)


def solution(mesh):
    return jax.shard_map(
        shards,
        mesh=mesh,
        in_specs=(P(None, "inline", "xline"),),
        out_specs=P(None, AXES),
        check_vma=False,
    )
```

```python
import functools
import math

import jax
import jax.numpy as jnp
import numpy as np
from jax import lax
from jax.experimental import pallas as pl
from jax.experimental.pallas import tpu as pltpu
from jax.sharding import PartitionSpec as P

NF = 256
COLS = 256
GC = 4
N_INLINE = 32
N_XLINE = 16
KAPPA = 40.0
AXES = ("inline", "xline")
F32 = jnp.float32
BF16 = jnp.bfloat16

ROOT = math.sqrt(0.5)
NODES = 0.5 * np.array([1.0, ROOT, 0.0, -ROOT, -1.0])


def basis_at(points):
    rows = []
    for k in range(5):
        factor = np.ones_like(points)
        for j in range(5):
            if j != k:
                factor = factor * (points - NODES[j]) / (NODES[k] - NODES[j])
        rows.append(factor)
    return np.stack(rows)


CHILD = [basis_at((t - 0.5) * 0.5 + 0.5 * NODES) for t in (0, 1)]
LEAF_XLINE = basis_at((np.arange(GC) + 0.5) / GC - 0.5)


FIRST_LEAD = 15
LEAD = 25


def wanted(index, place):
    return (index ^ LEAD) >> place & 1


def gather_groups():
    groups = []
    for base in range(N_INLINE * N_XLINE):
        a, b = base // N_XLINE, base % N_XLINE
        if a & 3 or b & 3:
            continue
        members = []
        for j in range(16):
            a0, b0, a1, b1 = (((j ^ FIRST_LEAD) >> place) & 1 for place in (3, 2, 1, 0))
            members.append((a | a0 | a1 << 1) * N_XLINE + (b | b0 | b1 << 1))
        groups.append(members)
    return groups


def scatter_groups():
    groups = []
    for base in range(N_INLINE * N_XLINE):
        a, b = base // N_XLINE, base % N_XLINE
        if a >> 2 or b >> 2:
            continue
        members = []
        for j in range(32):
            k6, k7, k5, k3, k4 = (wanted(j, place) for place in (4, 3, 2, 1, 0))
            members.append(
                (a | k3 << 2 | k5 << 3 | k7 << 4) * N_XLINE + (b | k4 << 2 | k6 << 3)
            )
        groups.append(members)
    return groups


def series(scale, bound, odd):
    coefs = []
    n = 0
    while True:
        power = 2 * n + (1 if odd else 0)
        size = (scale * bound) ** power / math.factorial(power)
        if size < 3e-8:
            return coefs
        coefs.append((-1.0) ** n * scale**power / math.factorial(power))
        n += 1


def poly(coefs, square):
    total = square * coefs[-1] + coefs[-2]
    for coef in coefs[-3::-1]:
        total = total * square + coef
    return total


def sincos_small(r, scale, bound):
    square = r * r
    return r * poly(series(scale, bound, True), square), poly(series(scale, bound, False), square)


def sincos_wide(x):
    turns = jnp.floor(x * (2.0 / math.pi) + 0.5)
    r = x - turns * 1.5703125
    r = r - turns * 4.837512969970703125e-4
    r = r - turns * 7.54978995489188216e-8
    sine, cosine = sincos_small(r, 1.0, 0.8)
    quarter = turns.astype(jnp.int32)
    swap = (quarter & 1) == 1
    s = jnp.where(swap, cosine, sine)
    c = jnp.where(swap, sine, cosine)
    s = jnp.where((quarter & 2) == 2, -s, s)
    c = jnp.where(((quarter + 1) & 2) == 2, -c, c)
    return s, c


def cmul(ar, ai, br, bi):
    return ar * br - ai * bi, ar * bi + ai * br


def full(value):
    return jnp.full((8, 128), value, F32)


def spot(bit):
    return (2 * bit - 1).astype(F32)


def places(where):
    a, b = where()
    lane = lax.broadcasted_iota(jnp.int32, (8, 128), 1)
    sub = lax.broadcasted_iota(jnp.int32, (8, 128), 0)
    column = lane + ((a & 1) << 7)

    def digits(where):
        coord = full(0.5 * 0.5 ** len(where))
        for rank, place in enumerate(where):
            coord = coord + (column >> place & 1).astype(F32) * 0.5 ** (rank + 1)
        return coord

    return a, b, lane, sub, (digits((7, 4, 1)), digits((6, 3, 0)), digits((5, 2)))


def five(factor):
    c1, s1, cv, sv = factor
    c2 = c1 * c1 - s1 * s1
    s2 = c1 * s1
    s2 = s2 + s2
    c3, s3 = cmul(c2, s2, c1, s1)
    cc, ss, cs, sc = c2 * cv, s2 * sv, c2 * sv, s2 * cv
    return [(c3, s3), (cc - ss, sc + cs), (c2, s2), (cc + ss, sc - cs), (c1, s1)]


NEAR = 11
STRETCHES = ((0, 7), (7, 11), (11, 15), (15, 19))


def stretch(k, table, held, sem, out):
    low, high = STRETCHES[k]
    far = table.at[pl.ds(low * 100, (high - low) * 100)]
    near = held.at[pl.ds(low * 100, (high - low) * 100)]
    return pltpu.make_async_copy(near, far, sem) if out else pltpu.make_async_copy(far, near, sem)


def plan(a, b, sub, centre):
    g0, g1, g2 = centre
    bit2, bit1, bit0, none = sub >> 2 & 1, sub >> 1 & 1, sub & 1, sub * 0
    a_base = a & ~3
    b_base = b & ~3
    unit_b = (b_base + bit2 + 2 * bit0).astype(F32) * (1.0 / N_XLINE)
    unit_a = (a_base + 2 * bit1).astype(F32) * (1.0 / N_INLINE)
    low_b = (b_base + 2 * bit0).astype(F32) * (1.0 / N_XLINE)

    def inline_low(bits):
        return (none + (a >> bits << bits)).astype(F32) * (1.0 / N_INLINE)

    def xline_low(bits):
        return (none + (b >> bits << bits)).astype(F32) * (1.0 / N_XLINE)

    levels = []
    sign = spot(none + (b & 1))
    for side in range(2):
        box = (unit_a + side / N_INLINE, 1.0 / N_INLINE, unit_b, 1.0 / N_XLINE)
        levels.append((box, (g0, g1, g2), 2, 2.0**-4, [sign], side))
    g2 = g2 + sign * 2.0**-4
    sign = spot(none + (a >> 1 & 1))
    box = (unit_a, 2.0 / N_INLINE, unit_b, 1.0 / N_XLINE)
    levels.append((box, (g0, g1, g2), 0, 2.0**-5, [sign], 0))
    g0 = g0 + sign * 2.0**-5
    sign = spot(none + (b >> 1 & 1))
    box = (unit_a, 2.0 / N_INLINE, low_b, 2.0 / N_XLINE)
    levels.append((box, (g0, g1, g2), 1, 2.0**-5, [sign], 1))
    g1 = g1 + sign * 2.0**-5
    sign = spot(bit1 ^ wanted(0, 1))
    box = (inline_low(2), 4.0 / N_INLINE, low_b, 2.0 / N_XLINE)
    levels.append((box, (g0, g1, g2), 2, 2.0**-5, [sign], 2))
    g2 = g2 + sign * 2.0**-5
    sign = spot(bit0 ^ wanted(0, 0))
    box = (inline_low(2), 4.0 / N_INLINE, xline_low(2), 4.0 / N_XLINE)
    levels.append((box, (g0, g1, g2), 0, 2.0**-6, [sign], 3))
    g0 = g0 + sign * 2.0**-6
    sign = spot(bit2 ^ wanted(0, 2))
    box = (inline_low(3), 8.0 / N_INLINE, xline_low(2), 4.0 / N_XLINE)
    levels.append((box, (g0, g1, g2), 1, 2.0**-6, [sign], 4))
    g1 = g1 + sign * 2.0**-6
    box = (inline_low(3), 8.0 / N_INLINE, xline_low(3), 8.0 / N_XLINE)
    signs = [2.0 * wanted(k << 4, 4) - 1.0 for k in range(2)]
    levels.append((box, (g0, g1, g2), 2, 2.0**-6, signs, 5))
    next_signs = [2.0 * wanted(k << 3, 3) - 1.0 for k in range(2)]
    for k6 in range(2):
        box = (inline_low(4), 16.0 / N_INLINE, xline_low(3), 8.0 / N_XLINE)
        centre = (g0, g1, g2 + signs[k6] * 2.0**-6)
        levels.append((box, centre, 0, 2.0**-7, next_signs, 7 + 2 * k6))
    for k6 in range(2):
        for k7 in range(2):
            box = (inline_low(4), 16.0 / N_INLINE, full(0.0), 16.0 / N_XLINE)
            centre = (g0 + next_signs[k7] * 2.0**-7, g1, g2 + signs[k6] * 2.0**-6)
            levels.append((box, centre, 1, 2.0**-7, [-1.0, 1.0], 11 + 4 * k6 + 2 * k7))
    return levels


def turning(level, slot, p_ref, q_ref, s_ref, store, part=None):
    (low0, width0, low1, width1), centre, dim, q, signs, first = level
    anchor = 0.5 + centre[0]
    for k in range(5):
        place = float(NODES[k]) + 0.5
        x0 = (low0 + width0 * place) * (low0 + width0 * place)
        x1 = (low1 + width1 * place) * (low1 + width1 * place)
        p_ref[slot, k] = anchor * anchor + centre[1] * x0
        q_ref[slot, k] = centre[2] * x1
        if dim:
            s_ref[slot, k] = (x0 if dim == 1 else x1) * q
    for m, sign in enumerate(signs):
        if dim == 0:
            s_ref[slot, m] = 2.0 * q * sign * anchor + q * q

    def point(b0, b1):
        radicand = p_ref[slot, b0] + q_ref[slot, b1]
        root = radicand * lax.rsqrt(radicand)
        for m, sign in enumerate(signs):
            if dim == 0:
                moved = radicand + s_ref[slot, m]
            else:
                gap = s_ref[slot, b0 if dim == 1 else b1]
                if isinstance(sign, float):
                    moved = radicand + gap if sign > 0 else radicand - gap
                else:
                    moved = radicand + sign * gap
            change = moved * lax.rsqrt(moved) - root
            if part is not None:
                change = change * part
            s_u, c_u = sincos_small(change, 0.5 * KAPPA, q)
            s_v, c_v = sincos_small(change, KAPPA * float(NODES[1]), q)
            store(first + m, b0, b1, (c_u, s_u, c_v, s_v))

    return point


def table_kernel(where, near_ref, turn_ref, far_ref, table_ref, tab_ref, far_s, table_s, p_ref, q_ref, s_ref, sems):
    a, b, lane, sub, (g0, g1, g2) = places(where)
    bit2 = sub >> 2 & 1
    bit1 = sub >> 1 & 1
    bit0 = sub & 1
    a_base = a & ~3
    b_base = b & ~3

    for half in range(2):
        box_a = (a_base + half + 2 * bit1).astype(F32)
        box_b = (b_base + bit2 + 2 * bit0).astype(F32)
        x0 = (box_a + 0.5) * (1.0 / N_INLINE)
        part = (0.5 + g0) * (0.5 + g0) + g1 * (x0 * x0)
        for c in range(GC):
            at = pl.ds(c * 16 + half * 8, 8)
            x1 = (box_b + (c + 0.5) / GC) * (1.0 / N_XLINE)
            radicand = part + g2 * (x1 * x1)
            step = (KAPPA / NF) * (radicand * lax.rsqrt(radicand))
            tab_ref[0, at, :] = step
            s, co = sincos_wide(step * 132.0)
            s64, c64 = sincos_wide(step * 64.0)
            for f1 in range(4):
                turn_ref[f1 * 16 + c * 2 + half] = co
                turn_ref[f1 * 16 + 8 + c * 2 + half] = s
                if f1 < 3:
                    co, s = cmul(co, s, c64, s64)
            s8, c8 = sincos_wide(step * 8.0)
            co, s = c8, s8
            for f2 in range(1, 8):
                tab_ref[2 * f2 - 1, at, :] = co
                tab_ref[2 * f2, at, :] = s
                if f2 < 7:
                    co, s = cmul(co, s, c8, s8)

    offset = sub.astype(F32) - 3.5

    def wave(box, ref, first):
        for c in range(GC):
            row = c * 16 + box

            def table(i):
                return jnp.broadcast_to(tab_ref[i, pl.ds(row, 1), :], (8, 128))

            s_a, c_a = sincos_small(table(0) * offset, 1.0, 1.15)
            cos_rows, sin_rows = [c_a], [s_a]
            for f2 in range(1, 8):
                cr, sr = cmul(c_a, s_a, table(2 * f2 - 1), table(2 * f2))
                cos_rows.append(cr)
                sin_rows.append(sr)
            right = jnp.concatenate(cos_rows + sin_rows, axis=0)
            right_hi = right.astype(BF16)
            ref[(box - first) * GC + c, 0:128, :] = right_hi
            ref[(box - first) * GC + c, 128:256, :] = (right - right_hi.astype(F32)).astype(BF16)

    def far_wave(box, carry):
        wave(box, far_s, NEAR)
        return carry

    def near_wave(box, carry):
        wave(box, near_ref, 0)
        return carry

    lax.fori_loop(NEAR, 16, far_wave, 0, unroll=True)
    save_far = pltpu.make_async_copy(far_s, far_ref, sems.at[4])
    save_far.start()

    def held(index, b0, b1, factor):
        for k in range(4):
            table_s[index * 100 + (b0 * 5 + b1) * 4 + k] = factor[k]

    saves = []
    part = jnp.where(bit2 == 1, 1.0, -1.0)
    for i, level in enumerate(plan(a, b, sub, (g0, g1, g2))[2:]):
        point = turning(level, 0, p_ref, q_ref, s_ref, held, part if i in (1, 2, 3) else None)

        def across(b1, carry, point=point):
            for b0 in range(5):
                point(b0, b1)
            return carry

        lax.fori_loop(0, 5, across, 0, unroll=True)
        if i in (5, 7, 9, 11):
            k = (i - 5) // 2
            saves.append(stretch(k, table_ref, table_s, sems.at[k], True))
            saves[-1].start()
    lax.fori_loop(0, NEAR, near_wave, 0, unroll=True)
    save_far.wait()
    for copy in saves:
        copy.wait()


def kernel(where, rows_ref, near_ref, turn_ref, far_ref, table_ref, out_ref, v_ref, leaf_ref, wa_ref, wb_ref, x_ref, far_s, table_s, first_s, p_ref, q_ref, s_ref, sems):
    load_far = pltpu.make_async_copy(far_ref, far_s, sems.at[4])
    load_far.start()
    loads = [stretch(k, table_ref, table_s, sems.at[k], False) for k in range(4)]
    for load in loads:
        load.start()
    a, b, lane, sub, kept = places(where)

    def hold_first(side, b0, b1, factor):
        for k in range(4):
            first_s[side * 20 + b1 * 4 + k] = factor[k]

    def hold(index, b0, b1, factor):
        for k in range(4):
            table_s[index * 100 + (b0 * 5 + b1) * 4 + k] = factor[k]

    upper = (sub >> 2 & 1) == 1
    part = jnp.where(upper, 1.0, -1.0)

    points = []
    for i, level in enumerate(plan(a, b, sub, kept)[:2]):
        point = turning(
            level, i, p_ref, q_ref, s_ref, hold_first if i < 2 else hold, part if i in (3, 4, 5) else None
        )
        points += [(point, b0, b1) for b0 in ((2,) if i < 2 else range(5)) for b1 in range(5)]

    left = lax.broadcasted_iota(jnp.int32, (16, 8, 128), 2) < 64
    re = rows_ref[:, 0:8, :]
    im = rows_ref[:, 8:16, :]
    re_r = pltpu.roll(re, 64, 2)
    im_r = pltpu.roll(im, 64, 2)
    v_ref[0, 0] = jnp.where(left, re, -im_r)
    v_ref[1, 0] = jnp.where(left, re_r, -im)
    v_ref[0, 1] = jnp.where(left, im, re_r)
    v_ref[1, 1] = jnp.where(left, im_r, re)

    basis = []
    for f1 in range(4):
        z = ((lane & 63).astype(F32) + (f1 * 64 + 0.5)) * (1.0 / NF) - 0.5
        factor = jnp.zeros((8, 128), F32)
        for k in range(5):
            scale = 1.0
            for j in range(5):
                if j != k:
                    scale = scale / (NODES[k] - NODES[j])
            factor = jnp.where(sub == k, scale, factor)
        for j in range(5):
            factor = factor * jnp.where(sub == j, 1.0, z - NODES[j])
        basis.append(factor)

    def leaf_one(box):
        totals = []
        for c in range(GC):
            def table(i):
                return jnp.broadcast_to(turn_ref[i * 8 + c * 2 + box // 8, pl.ds(box % 8, 1), :], (8, 128))

            rows = []
            for f1 in range(4):
                for part in range(2):
                    sample = v_ref[f1 & 1, part, pl.ds(box ^ FIRST_LEAD, 1), 2 * c + f1 // 2, :]
                    rows.append(basis[f1] * jnp.broadcast_to(sample, (8, 128)))
            lhs = jnp.concatenate(rows, axis=0)
            lhs_hi = lhs.astype(BF16)
            lhs_lo = (lhs - lhs_hi.astype(F32)).astype(BF16)
            both = jnp.concatenate([lhs_hi, lhs_hi], axis=1)
            right = near_ref[box * GC + c] if box < NEAR else far_s[(box - NEAR) * GC + c]
            mixed = jnp.dot(both, right, preferred_element_type=F32)
            mixed = mixed + jnp.dot(lhs_lo, right[0:128], preferred_element_type=F32)
            t_re = None
            for f1 in range(4):
                u_re = mixed[f1 * 16 : f1 * 16 + 8]
                u_im = mixed[f1 * 16 + 8 : f1 * 16 + 16]
                r_re, r_im = cmul(u_re, u_im, table(2 * f1), table(2 * f1 + 1))
                t_re, t_im = (r_re, r_im) if t_re is None else (t_re + r_re, t_im + r_im)
            totals.append((t_re, t_im))
        for a1 in range(5):
            for part in range(2):
                total = totals[0][part] * float(LEAF_XLINE[a1, 0])
                for c in range(1, GC):
                    total = total + totals[c][part] * float(LEAF_XLINE[a1, c])
                leaf_ref[pl.ds((a1 * 16 + part) * 16 + box, 8, stride=32), :] = total

    for box in range(16):
        if box == NEAR:
            load_far.wait()
        leaf_one(box)
        for point, b0, b1 in points[box::16]:
            point(b0, b1)

    def merge(axis, points, sets, read, turn, weight, write):
        def body(other, carry):
            for n, (side, p) in enumerate(points):
                b0, b1 = (p, other) if axis == 0 else (other, p)
                turns = [five(turn(m, side, b0, b1)) for m in range(sets)]
                for b2 in range(5):
                    w_re, w_im = read(side, b0, b1, b2)
                    for m in range(sets):
                        x_re, x_im = cmul(w_re, w_im, *turns[m][b2])
                        x_ref[(m * 5 + n) * 10 + 2 * b2] = x_re
                        x_ref[(m * 5 + n) * 10 + 2 * b2 + 1] = x_im
            for m in range(sets):
                for b2 in range(5):
                    items = [
                        [x_ref[(m * 5 + n) * 10 + 2 * b2 + k] for n in range(len(points))] for k in range(2)
                    ]
                    for i in range(5):
                        totals = []
                        for k in range(2):
                            total = None
                            for (side, p), item in zip(points, items[k]):
                                coef = weight(i, side, p)
                                if coef is None:
                                    continue
                                term = item if isinstance(coef, float) and coef == 1.0 else item * coef
                                total = term if total is None else total + term
                            totals.append(total)
                        i0, i1 = (i, other) if axis == 0 else (other, i)
                        write(m, i0, i1, b2, totals)
            return carry

        lax.fori_loop(0, 5, body, 0)

    def merge_packed(axis, weight, read, turn, write, combine):
        def body(other, carry):
            for b in range(5):
                b0, b1 = (b, other) if axis == 0 else (other, b)
                for b2, (co, sine) in enumerate(five(turn(0, 0, b0, b1))):
                    both = read(b0, b1, b2)
                    x_ref[b * 5 + b2] = both * co + pltpu.roll(both, 4, 0) * sine
            for b2 in range(5):
                items = [x_ref[b * 5 + b2] for b in range(5)]
                for i in range(5):
                    total = None
                    for b in range(5):
                        coef = weight(i, 0, b)
                        if coef is None:
                            continue
                        term = items[b] if isinstance(coef, float) and coef == 1.0 else items[b] * coef
                        total = term if total is None else total + term
                    i0, i1 = (i, other) if axis == 0 else (other, i)
                    write(i0, i1, b2, combine(total))
            return carry

        lax.fori_loop(0, 5, body, 0)

    def packed_reader(ref, order=None):
        def read(b0, b1, b2):
            b0, b1 = (b0, b1) if order is None else order(b0, b1)
            return ref[0, (b0 * 5 + b1) * 10 + b2]

        return read

    def packed_writer(ref, order=None):
        def write(i0, i1, b2, value):
            i0, i1 = (i0, i1) if order is None else order(i0, i1)
            ref[0, (i0 * 5 + i1) * 10 + b2] = value

        return write

    def unpacked_reader(ref, order):
        def read(side, b0, b1, b2):
            b0, b1 = order(b0, b1)
            both = ref[0, (b0 * 5 + b1) * 10 + b2]
            turned = pltpu.roll(both, 4, 0)
            return jnp.where(upper, turned, both), jnp.where(upper, both, turned)

        return read

    def chosen(mask):
        table = [
            [
                None
                if CHILD[0][i, j] == 0.0 and CHILD[1][i, j] == 0.0
                else jnp.where(mask, float(CHILD[1][i, j]), float(CHILD[0][i, j]))
                for j in range(5)
            ]
            for i in range(5)
        ]
        return lambda i, side, j: table[i][j]

    def lower(i, side, j):
        return None if CHILD[0][i, j] == 0.0 else float(CHILD[0][i, j])

    def flipped(axis, bit):
        def order(i0, i1):
            if axis == 0:
                return i0 + bit * (4 - 2 * i0), i1
            return i0, i1 + bit * (4 - 2 * i1)

        return order

    def same(i0, i1):
        return i0, i1

    def reader(ref, index, order=same):
        def read(side, b0, b1, b2):
            b0, b1 = order(b0, b1)
            at = (b0 * 5 + b1) * 10 + b2 * 2
            return ref[index, at], ref[index, at + 1]

        return read

    def turner(index_of, order=same):
        def turn(m, side, b0, b1):
            b0, b1 = order(b0, b1)
            at = index_of(m) * 100 + (b0 * 5 + b1) * 4
            return [table_s[at + k] for k in range(4)]

        return turn

    def writer(ref, index_of, order=same):
        def write(m, i0, i1, b2, totals):
            i0, i1 = order(i0, i1)
            for k in range(2):
                ref[index_of(m), (i0 * 5 + i1) * 10 + 2 * b2 + k] = totals[k]

        return write

    line = [(0, j) for j in range(5)]

    def leaf_read(side, b0, b1, b2):
        base = pl.multiple_of((b1 * 8 + b2) * 32 + side * 8, 8)
        return leaf_ref[pl.ds(base, 8), :], leaf_ref[pl.ds(base + 16, 8), :]

    merge(
        0, [(0, 2), (1, 2)], 1, leaf_read,
        lambda m, side, b0, b1: [first_s[side * 20 + b1 * 4 + k] for k in range(4)],
        lambda i, side, j: float(CHILD[side][i, j]),
        writer(wa_ref, lambda m: 0),
    )
    loads[0].wait()
    def pack(m, i0, i1, b2, totals):
        re, im = totals
        both = jnp.where(upper, im, re) + pltpu.roll(jnp.where(upper, re, im), 4, 0)
        wb_ref[0, (i0 * 5 + i1) * 10 + b2] = both

    merge(1, line, 1, reader(wa_ref, 0), turner(lambda m: 0), chosen(upper), pack)
    odd = (sub >> 1 & 1) == 1
    merge_packed(
        0, chosen(odd), packed_reader(wb_ref), turner(lambda m: 1), packed_writer(wa_ref),
        lambda v: v + jnp.where(odd, pltpu.roll(v, 2, 0), pltpu.roll(v, 6, 0)),
    )
    even = (sub & 1) == 0
    merge_packed(
        1, chosen((sub & 1) == 1), packed_reader(wa_ref), turner(lambda m: 2), packed_writer(wb_ref),
        lambda v: v + jnp.where(even, pltpu.roll(v, 7, 0), pltpu.roll(v, 1, 0)),
    )
    order = flipped(0, a >> 2 & 1)
    merge_packed(
        0, lower, packed_reader(wb_ref, order), turner(lambda m: 3, order), packed_writer(wa_ref, order),
        lambda v: v,
    )
    order = flipped(1, b >> 2 & 1)
    merge(
        1, line, 1, unpacked_reader(wa_ref, order), turner(lambda m: 4, order), lower,
        writer(wb_ref, lambda m: 0, order),
    )
    order = flipped(0, a >> 3 & 1)
    merge(
        0, line, 2, reader(wb_ref, 0, order), turner(lambda m: 5 + m, order), lower,
        writer(wa_ref, lambda m: m, order),
    )
    loads[1].wait()
    order = flipped(1, b >> 3 & 1)
    for k6 in range(2):
        merge(
            1, line, 2, reader(wa_ref, k6, order),
            turner((lambda k6: lambda m: 7 + 2 * k6 + m)(k6), order), lower,
            writer(wb_ref, (lambda k6: lambda m: 2 * k6 + m)(k6), order),
        )

    loads[2].wait()
    loads[3].wait()
    scale = 1.0 / math.sqrt(GC * NF * N_INLINE * N_XLINE)
    for k67 in range(4):
        read = reader(wb_ref, k67)

        def body(b0, sums, k67=k67, read=read):
            sums = list(sums)
            for b1 in range(5):
                w = [read(0, b0, b1, b2) for b2 in range(5)]
                wp_re, wp_im = w[1][0] + w[3][0], w[1][1] + w[3][1]
                wm_re, wm_im = w[1][0] - w[3][0], w[1][1] - w[3][1]
                for m in range(2):
                    cu, su, cv, sv = (table_s[(11 + 2 * k67 + m) * 100 + (b0 * 5 + b1) * 4 + k] for k in range(4))
                    t_re, t_im = cmul(w[0][0], w[0][1], cu, su)
                    t_re = t_re + (w[2][0] + (cv * wp_re - sv * wm_im))
                    t_im = t_im + (w[2][1] + (cv * wp_im + sv * wm_re))
                    t_re, t_im = cmul(t_re, t_im, cu, su)
                    t_re, t_im = cmul(t_re + w[4][0], t_im + w[4][1], cu, su)
                    sums[2 * m] = sums[2 * m] + t_re
                    sums[2 * m + 1] = sums[2 * m + 1] + t_im
            return tuple(sums)

        sums = lax.fori_loop(0, 5, body, tuple(full(0.0) for _ in range(4)))
        for m in range(2):
            for part in range(2):
                out_ref[pl.ds(k67 * 32 + part * 2 + m, 8, stride=4), :] = sums[2 * m + part] * scale


def in_vmem():
    return pl.BlockSpec(memory_space=pltpu.VMEM)


def in_hbm():
    return pl.BlockSpec(memory_space=pltpu.HBM)


def device_place():
    return lax.axis_index("inline"), lax.axis_index("xline")


def told(body):
    def with_place(where_ref, *refs):
        body(lambda: (where_ref[0], where_ref[1]), *refs)

    return with_place


def run(body, where, in_specs, operands, **settings):
    if where is None:
        return pl.pallas_call(functools.partial(body, device_place), in_specs=in_specs, **settings)(*operands)
    return pl.pallas_call(
        told(body), in_specs=[pl.BlockSpec(memory_space=pltpu.SMEM)] + in_specs, interpret=True, **settings
    )(where, *operands)


def tables(where):
    return run(
        table_kernel,
        where,
        [],
        [],
        out_shape=[
            jax.ShapeDtypeStruct((NEAR * GC, 256, 128), BF16),
            jax.ShapeDtypeStruct((64, 8, 128), F32),
            pltpu.HBM(((16 - NEAR) * GC, 256, 128), BF16),
            pltpu.HBM((1900, 8, 128), F32),
        ],
        out_specs=[in_vmem(), in_vmem(), in_hbm(), in_hbm()],
        scratch_shapes=[
            pltpu.VMEM((15, 64, 128), F32),
            pltpu.VMEM(((16 - NEAR) * GC, 256, 128), BF16),
            pltpu.VMEM((1900, 8, 128), F32),
            pltpu.VMEM((1, 5, 8, 128), F32),
            pltpu.VMEM((1, 5, 8, 128), F32),
            pltpu.VMEM((1, 5, 8, 128), F32),
            pltpu.SemaphoreType.DMA((5,)),
        ],
        compiler_params=pltpu.CompilerParams(vmem_limit_bytes=14 << 20),
    )


def contributions(where, rows):
    near, turn, far, table = tables(where)
    if where is None:
        far = pltpu.with_memory_space_constraint(far, pltpu.HBM)
        table = pltpu.with_memory_space_constraint(table, pltpu.HBM)
    return run(
        kernel,
        where,
        [in_vmem(), in_vmem(), in_vmem(), in_hbm(), in_hbm()],
        [rows, near, turn, far, table],
        out_shape=jax.ShapeDtypeStruct((128, 128), F32),
        out_specs=in_vmem(),
        scratch_shapes=[
            pltpu.VMEM((2, 2, 16, 8, 128), F32),
            pltpu.VMEM((1280, 128), F32),
            pltpu.VMEM((2, 250, 8, 128), F32),
            pltpu.VMEM((4, 250, 8, 128), F32),
            pltpu.VMEM((100, 8, 128), F32),
            pltpu.VMEM(((16 - NEAR) * GC, 256, 128), BF16),
            pltpu.VMEM((1900, 8, 128), F32),
            pltpu.VMEM((40, 8, 128), F32),
            pltpu.VMEM((8, 5, 8, 128), F32),
            pltpu.VMEM((8, 5, 8, 128), F32),
            pltpu.VMEM((8, 5, 8, 128), F32),
            pltpu.SemaphoreType.DMA((5,)),
        ],
        compiler_params=pltpu.CompilerParams(vmem_limit_bytes=20 << 20),
    )


def shards(samples):
    rows = samples.reshape(1, 16, 128)
    rows = jnp.broadcast_to(rows, (16, 16, 128))
    rows = lax.all_to_all(rows, AXES, 0, 0, axis_index_groups=gather_groups())
    parts = contributions(None, rows).reshape(32, 4, 128)
    parts = lax.all_to_all(parts, AXES, 0, 0, axis_index_groups=scatter_groups())
    return jnp.sum(parts, axis=0).reshape(2, COLS)


def solution(mesh):
    return jax.shard_map(
        shards,
        mesh=mesh,
        in_specs=(P(None, "inline", "xline"),),
        out_specs=P(None, AXES),
        check_vma=False,
    )
```
